256 devices in a mesh: seq: 32 (over z, x), head: 8 (over y, core).
Axes of the slice: x: 4, y: 4, z: 8, core: 2. Of those that a mesh axis runs over, the one named last changes fastest.
Arguments:
- queries: bfloat16 [8192, 1024], P('seq', 'head'), may hold values from -16 to 16
- keys: bfloat16 [8192, 1024], P(('seq', 'head')), may hold values from -16 to 16
- values: bfloat16 [8192, 1024], P(('seq', 'head')), may hold values from -6 to 6
- out_grad: bfloat16 [8192, 1024], P('seq', 'head'), may hold values from -6 to 6
Outputs:
- attended: bfloat16 [8192, 1024], P('seq', 'head')
- query_grad: float32 [8192, 1024], P('seq', 'head')
- key_grad: float32 [8192, 1024], P('seq', 'head')
- value_grad: float32 [8192, 1024], P('seq', 'head')
The draws below stay inside these ranges and needn't reach their ends.
All inputs are finite; a program needn't handle non-finite values.
Results may differ from the reference program's by a relative error of at most 0.0095.
Values may be sent and summed in bfloat16 or wider, within the bound.
No kernel may reach another device: no remote copies, remote signals or barrier semaphores. Data moves between devices by JAX's collectives and lax.ppermute only.
A program may use at most 64 MiB of HBM per device.

```python
import math
import jax
import jax.numpy as jnp
from jax import lax

HEAD_DIM = 128
HEADS = 8
TOKENS = 8192


def query_key_pair(key):
    columns = HEADS * HEAD_DIM
    query_base = jax.random.normal(jax.random.fold_in(key, 101), (TOKENS, columns), jnp.float32)
    key_base = jax.random.normal(jax.random.fold_in(key, 202), (TOKENS, columns), jnp.float32)
    query_out = query_base * 3.0
    key_out = key_base
    return (jnp.clip(query_out, -16.0, 16.0), jnp.clip(key_out, -16.0, 16.0))


def draw_queries(key, part):
    pair = query_key_pair(key)
    return pair[0].astype(jnp.bfloat16)


def draw_keys(key, part):
    pair = query_key_pair(key)
    return pair[1].astype(jnp.bfloat16)


def levels(stream_key, shape, cuts, least, high):
    gain, own = 1.0, jax.random.fold_in(stream_key, 6)
    for dim, shards_of in cuts:
        heights = jnp.exp(jax.random.uniform(jax.random.fold_in(own, dim), (shards_of,), jnp.float32, least / len(cuts), high / len(cuts)))
        gain = gain * jnp.repeat(heights, shape[dim] // shards_of).reshape([-1 if axis == dim else 1 for axis in range(len(shape))])
    return gain


def normal_values(stream_key, shape, width, reach, cuts=(), held_as=jnp.bfloat16):
    result = width * jax.random.normal(stream_key, shape, jnp.float32)
    if cuts:
        result = result * levels(stream_key, shape, cuts, -0.22, 0.18)
    return jnp.clip(result, -reach, reach).astype(held_as)


def setup_inputs(seed: int = 0) -> dict:
    streams_of = jax.random.split(jax.random.key(seed), 5)
    return {
        "queries": draw_queries(jax.random.fold_in(streams_of[4], 71), 0),
        "keys": draw_keys(jax.random.fold_in(streams_of[4], 71), 0),
        "values": normal_values(streams_of[2], (TOKENS, HEADS * HEAD_DIM), 1.0, 6.0, ((0, 256),)),
        "out_grad": normal_values(streams_of[3], (TOKENS, HEADS * HEAD_DIM), 1.0, 6.0, ((0, 32), (1, 8))),
    }


masked_value = -1e+30

def one_head(queries, keys, values, out_grad):
    length, head_width = queries.shape
    scaling = 1.0 / math.sqrt(head_width)
    span_rows = min(length, 512)
    span_count = length // span_rows
    key_pos = jnp.arange(length, dtype=jnp.int32)

    def forward(unused, number):
        qstart = (number * span_rows).astype(jnp.int32)
        query_piece = lax.dynamic_slice_in_dim(queries, qstart, span_rows, 0)
        query_pos = qstart + jnp.arange(span_rows, dtype=jnp.int32)
        allowed = key_pos[None, :] <= query_pos[:, None]
        scores = jnp.dot(query_piece, keys.T, preferred_element_type=jnp.float32) * scaling
        scores = jnp.where(allowed, scores, masked_value)
        rowmax = lax.optimization_barrier(jnp.max(scores, axis=1))
        weights = jnp.where(allowed, jnp.exp(scores - rowmax[:, None]), 0.0)
        rowsum = lax.optimization_barrier(jnp.sum(weights, axis=1))
        weighted = jnp.dot(weights.astype(jnp.bfloat16), values, preferred_element_type=jnp.float32)
        return (unused, (weighted / rowsum[:, None], rowmax + jnp.log(rowsum)))
    numbers = jnp.arange(span_count, dtype=jnp.int32)
    unused, (pieces, norms) = lax.scan(forward, jnp.zeros((), jnp.float32), numbers)
    output = pieces.reshape(length, head_width)
    log_norm = norms.reshape(length)
    row_delta = lax.optimization_barrier(jnp.sum(out_grad.astype(jnp.float32) * output, axis=1))

    def backward(running, number):
        key_total, value_total = running
        qstart = (number * span_rows).astype(jnp.int32)
        query_piece = lax.dynamic_slice_in_dim(queries, qstart, span_rows, 0)
        grad_piece = lax.dynamic_slice_in_dim(out_grad, qstart, span_rows, 0)
        norm_piece = lax.dynamic_slice_in_dim(log_norm, qstart, span_rows, 0)
        delta_piece = lax.dynamic_slice_in_dim(row_delta, qstart, span_rows, 0)
        query_pos = qstart + jnp.arange(span_rows, dtype=jnp.int32)
        allowed = key_pos[None, :] <= query_pos[:, None]
        scores = jnp.dot(query_piece, keys.T, preferred_element_type=jnp.float32) * scaling
        probs = jnp.where(allowed, jnp.exp(scores - norm_piece[:, None]), 0.0)
        grad_probs = jnp.dot(grad_piece, values.T, preferred_element_type=jnp.float32)
        grad_scores = (probs * (grad_probs - delta_piece[:, None]) * scaling).astype(jnp.bfloat16)
        query_part = jnp.dot(grad_scores, keys, preferred_element_type=jnp.float32)
        key_total = key_total + jnp.dot(grad_scores.T, query_piece, preferred_element_type=jnp.float32)
        value_total = value_total + jnp.dot(probs.astype(jnp.bfloat16).T, grad_piece, preferred_element_type=jnp.float32)
        return ((key_total, value_total), query_part)
    initial = (jnp.zeros((length, head_width), jnp.float32), jnp.zeros((length, head_width), jnp.float32))
    (key_grad, value_grad), query_parts = lax.scan(backward, initial, numbers)
    query_grad = query_parts.reshape(length, head_width)
    return (output.astype(jnp.bfloat16), query_grad, key_grad, value_grad)

def reference(queries, keys, values, out_grad):
    outputs = []
    for head_number in range(HEADS):
        low_col = head_number * HEAD_DIM
        results = one_head(queries[:, low_col:low_col + HEAD_DIM], keys[:, low_col:low_col + HEAD_DIM], values[:, low_col:low_col + HEAD_DIM], out_grad[:, low_col:low_col + HEAD_DIM])
        outputs.append(results)
    attended = jnp.concatenate([item[0] for item in outputs], axis=1)
    query_grad = jnp.concatenate([item[1] for item in outputs], axis=1)
    key_grad = jnp.concatenate([item[2] for item in outputs], axis=1)
    value_grad = jnp.concatenate([item[3] for item in outputs], axis=1)
    return (attended, query_grad, key_grad, value_grad)
```

```python
import functools
import math

import jax
import jax.numpy as jnp
from jax import lax
from jax.experimental import pallas as pl
from jax.experimental.pallas import tpu as pltpu
from jax.sharding import Mesh
from jax.sharding import PartitionSpec as P

SEQ = ("z", "x")
SEQ_HEAD = ("z", "x", "head")
LOW = -1e30
F32 = jnp.float32
BF16 = jnp.bfloat16
NT = (((1,), (1,)), ((), ()))
TN = (((0,), (0,)), ((), ()))
NN = (((1,), (0,)), ((), ()))


def dot(a, b, dims):
    return lax.dot_general(a, b, dims, preferred_element_type=F32)


def allowed_pairs(rows, key_block, query_block):
    key_pos = lax.broadcasted_iota(jnp.int32, (rows, rows), 0) + key_block * rows
    query_pos = lax.broadcasted_iota(jnp.int32, (rows, rows), 1) + query_block * rows
    return key_pos <= query_pos


def forward_kernel(rate, nx, where_ref, *refs):
    q_refs, (kv_ref, o_ref, stat_ref, m_ref, l_ref) = refs[:nx], refs[nx:]
    z, x = where_ref[0], where_ref[1]
    rows, width = kv_ref.shape[1], kv_ref.shape[2] // 2
    m_ref[...] = jnp.full_like(m_ref, LOW)
    l_ref[...] = jnp.zeros_like(l_ref)
    o_ref[...] = jnp.zeros_like(o_ref)

    def unit(j, masked):
        k, v = kv_ref[j, :, :width], kv_ref[j, :, width:]
        for r in range(nx):
            cols = slice(r * rows, (r + 1) * rows)
            s = dot(k, q_refs[r][:, :width], NT)
            if masked:
                ok = allowed_pairs(rows, x, lax.rem(x - r + nx, nx))
                s = jnp.where(ok, s, LOW)
            m_old = m_ref[:, cols]
            m_new = jnp.maximum(m_old, jnp.max(s, axis=0, keepdims=True))
            p = jnp.exp2((s - m_new) * rate)
            if masked:
                p = jnp.where(ok, p, 0.0)
            alpha = jnp.exp2((m_old - m_new) * rate)
            m_ref[:, cols] = m_new
            l_ref[:, cols] = l_ref[:, cols] * alpha + jnp.sum(p, axis=0, keepdims=True)
            o_ref[:, cols] = o_ref[:, cols] * alpha + dot(v, p.astype(BF16), TN)

    @pl.loop(0, z)
    def _(j):
        unit(j, False)

    unit(z, True)
    for r in range(nx):
        cols = slice(r * rows, (r + 1) * rows)
        grads = jnp.transpose(q_refs[r][:, width:].astype(F32))
        at = lax.rem(x - r + nx, nx)
        stat_ref[at, 0:1, :] = m_ref[:, cols] * rate
        stat_ref[at, 1:2, :] = l_ref[:, cols]
        stat_ref[at, 2:3, :] = jnp.sum(grads * o_ref[:, cols], axis=0, keepdims=True)


def backward_kernel(rate, scaling, nx, where_ref, *refs):
    q_refs, (kv_ref, o_ref, stat_ref), refs = refs[:nx], refs[nx : nx + 3], refs[nx + 3 :]
    out_refs, (dkv_ref, dq_ref, norm_ref, delta_ref) = refs[:nx], refs[nx:]
    z, x = where_ref[0], where_ref[1]
    rows, width = kv_ref.shape[1], kv_ref.shape[2] // 2
    dq_ref[...] = jnp.zeros_like(dq_ref)
    for r in range(nx):
        cols = slice(r * rows, (r + 1) * rows)
        at = lax.rem(x - r + nx, nx)
        maxima = [stat_ref[i, at, 0:1, :] for i in range(nx)]
        top = functools.reduce(jnp.maximum, maxima)
        shares = [jnp.exp2(m - top) for m in maxima]
        total = sum(stat_ref[i, at, 1:2, :] * shares[i] for i in range(nx))
        delta = sum(stat_ref[i, at, 2:3, :] * shares[i] for i in range(nx))
        norm = top + jnp.log2(total)
        norm_ref[:, cols] = norm
        delta_ref[:, cols] = delta / total
        own = stat_ref[x, at, 0:1, :]
        mine = o_ref[:, cols] * (jnp.exp2(own - top) / total)
        out_refs[r][:, width:] = jnp.transpose(mine).astype(BF16)

    def unit(j, masked):
        k, v = kv_ref[j, :, :width], kv_ref[j, :, width:]
        dk = jnp.zeros((rows, width), F32)
        dv = jnp.zeros((rows, width), F32)
        for r in range(nx):
            cols = slice(r * rows, (r + 1) * rows)
            q, g = q_refs[r][:, :width], q_refs[r][:, width:]
            s = dot(k, q, NT)
            p = jnp.exp2(s * rate - norm_ref[:, cols])
            if masked:
                p = jnp.where(allowed_pairs(rows, x, lax.rem(x - r + nx, nx)), p, 0.0)
            ds = (p * (dot(v, g, NT) - delta_ref[:, cols])).astype(BF16)
            dv = dv + dot(p.astype(BF16), g, NN)
            dk = dk + dot(ds, q, NN)
            dq_ref[:, cols] += dot(k, ds, TN)
        dkv_ref[j, :, :width] = (dk * scaling).astype(BF16)
        dkv_ref[j, :, width:] = dv.astype(BF16)

    @pl.loop(0, z)
    def _(j):
        unit(j, False)

    unit(z, True)

    @pl.loop(z + 1, kv_ref.shape[0])
    def _(j):
        dkv_ref[j] = jnp.zeros(kv_ref.shape[1:], BF16)

    for r in range(nx):
        cols = slice(r * rows, (r + 1) * rows)
        out_refs[r][:, :width] = jnp.transpose(dq_ref[:, cols] * scaling).astype(BF16)


def shifted(value, axis, count, step):
    return lax.ppermute(value, axis, [(i, (i + step) % count) for i in range(count)])


def per_device(nz, nx, nh, queries, keys, values, out_grad):
    rows, width = queries.shape
    scaling = 1.0 / math.sqrt(width)
    rate = scaling * math.log2(math.e)
    smem = pl.BlockSpec(memory_space=pltpu.SMEM)
    vmem = pl.BlockSpec(memory_space=pltpu.VMEM)
    own = jnp.concatenate([queries, out_grad], axis=1)
    blocks = [own] + [shifted(own, "x", nx, r) for r in range(1, nx)]
    mixed = jnp.concatenate(
        [keys.reshape(-1, nh, width), values.reshape(-1, nh, width)], axis=2
    ).transpose(1, 0, 2)
    local = lax.all_to_all(mixed, "head", 0, 0, tiled=True).reshape(rows, 2 * width)
    kv = lax.all_to_all(jnp.broadcast_to(local, (nz, *local.shape)), "z", 0, 0, tiled=True)
    where = jnp.stack([lax.axis_index("z"), lax.axis_index("x")]).astype(jnp.int32)
    pairs = nz * rows * nx * rows * width
    partial, stats = pl.pallas_call(
        functools.partial(forward_kernel, rate, nx),
        out_shape=(
            jax.ShapeDtypeStruct((width, nx * rows), F32),
            jax.ShapeDtypeStruct((nx, 8, rows), F32),
        ),
        in_specs=[smem] + [vmem] * (nx + 1),
        out_specs=(vmem, vmem),
        scratch_shapes=[pltpu.VMEM((1, nx * rows), F32), pltpu.VMEM((1, nx * rows), F32)],
        cost_estimate=pl.CostEstimate(flops=4 * pairs, bytes_accessed=2 << 20, transcendentals=0),
        name="forward",
    )(where, *blocks, kv)
    stats = lax.all_to_all(jnp.broadcast_to(stats, (nx, *stats.shape)), "x", 0, 0, tiled=True)
    *parts, dkv = pl.pallas_call(
        functools.partial(backward_kernel, rate, scaling, nx),
        out_shape=tuple(jax.ShapeDtypeStruct((rows, 2 * width), BF16) for _ in range(nx))
        + (jax.ShapeDtypeStruct(kv.shape, BF16),),
        in_specs=[smem] + [vmem] * (nx + 3),
        out_specs=(vmem,) * (nx + 1),
        scratch_shapes=[
            pltpu.VMEM((width, nx * rows), F32),
            pltpu.VMEM((1, nx * rows), F32),
            pltpu.VMEM((1, nx * rows), F32),
        ],
        cost_estimate=pl.CostEstimate(flops=10 * pairs, bytes_accessed=2 << 20, transcendentals=0),
        name="backward",
    )(where, *blocks, kv, partial, stats)
    arrived = [shifted(parts[-r % nx], "x", nx, r) for r in range(1, nx)]
    dkv = lax.all_to_all(dkv, "z", 0, 0, tiled=True)
    dkv = jnp.sum(dkv.astype(F32), axis=0)
    total = functools.reduce(jnp.add, [a.astype(F32) for a in [parts[0], *arrived]])
    return total[:, width:].astype(BF16), total[:, :width], dkv[:, :width], dkv[:, width:]


def solution(mesh):
    nh = mesh.shape["head"]
    split = Mesh(mesh.devices.reshape(8, -1, nh), SEQ_HEAD)
    return jax.shard_map(
        functools.partial(per_device, 8, split.shape["x"], nh),
        mesh=split,
        in_specs=(P(SEQ, "head"), P(SEQ_HEAD, None), P(SEQ_HEAD, None), P(SEQ, "head")),
        out_specs=(P(SEQ, "head"),) * 4,
        check_vma=False,
    )
```

```python
import functools
import math

import jax
import jax.numpy as jnp
from jax import lax
from jax.experimental import pallas as pl
from jax.experimental.pallas import tpu as pltpu
from jax.sharding import Mesh
from jax.sharding import PartitionSpec as P

Z = ("zj", "zp")
SEQ = (*Z, "x")
VMEM = 24 << 20
LOW = -1e30
F32 = jnp.float32
BF16 = jnp.bfloat16
NT = (((1,), (1,)), ((), ()))
TN = (((0,), (0,)), ((), ()))
NN = (((1,), (0,)), ((), ()))


def dot(a, b, dims):
    return lax.dot_general(a, b, dims, preferred_element_type=F32)


def allowed_pairs(rows, key_block, query_block):
    key_pos = lax.broadcasted_iota(jnp.int32, (rows, rows), 0) + key_block * rows
    query_pos = lax.broadcasted_iota(jnp.int32, (rows, rows), 1) + query_block * rows
    return key_pos <= query_pos


def spans(where_ref):
    zj, zp = where_ref[0], where_ref[1]
    return zj, 4 - zp - zj


def forward_kernel(rate, nx, where_ref, *refs):
    q_refs, (kv_ref, o_ref, stat_ref, m_ref, l_ref) = refs[: 2 * nx], refs[2 * nx :]
    x, high = where_ref[2], where_ref[3]
    own, mirror = spans(where_ref)
    rows, width = kv_ref.shape[1], kv_ref.shape[2] // 2
    m_ref[...] = jnp.full_like(m_ref, LOW)
    l_ref[...] = jnp.zeros_like(l_ref)
    o_ref[...] = jnp.zeros_like(o_ref)

    def unit(side, j, masked):
        k, v = kv_ref[j, :, :width], kv_ref[j, :, width:]
        for r in range(nx):
            at = side * nx + r
            cols = slice(at * rows, (at + 1) * rows)
            s = dot(k, q_refs[at][:, :width], NT)
            if masked:
                ok = allowed_pairs(rows, x, lax.rem(x - r + nx, nx))
                s = jnp.where(ok, s, LOW)
            m_old = m_ref[:, cols]
            m_new = jnp.maximum(m_old, jnp.max(s, axis=0, keepdims=True))
            p = jnp.exp2((s - m_new) * rate)
            if masked:
                p = jnp.where(ok, p, 0.0)
            alpha = jnp.exp2((m_old - m_new) * rate)
            m_ref[:, cols] = m_new
            l_ref[:, cols] = l_ref[:, cols] * alpha + jnp.sum(p, axis=0, keepdims=True)
            o_ref[:, cols] = o_ref[:, cols] * alpha + dot(v, p.astype(BF16), TN)

    @pl.loop(0, own)
    def _(j):
        unit(0, j, False)

    unit(0, own, True)

    @pl.loop(0, mirror)
    def _(j):
        unit(1, j, False)

    for at in range(2 * nx):
        side, r = divmod(at, nx)
        cols = slice(at * rows, (at + 1) * rows)
        grads = jnp.transpose(q_refs[at][:, width:].astype(F32))
        to = lax.rem(x - r + nx, nx)
        end = side ^ high
        stat_ref[end, to, 0:1, :] = m_ref[:, cols] * rate
        stat_ref[end, to, 1:2, :] = l_ref[:, cols]
        stat_ref[end, to, 2:3, :] = jnp.sum(grads * o_ref[:, cols], axis=0, keepdims=True)


def backward_kernel(rate, scaling, nx, where_ref, *refs):
    n = 2 * nx
    q_refs, (kv_ref, o_ref, mine_ref, stat_ref), refs = refs[:n], refs[n : n + 4], refs[n + 4 :]
    out_refs, (dkv_ref, dq_ref, norm_ref, delta_ref, acc_ref) = refs[:nx], refs[nx:]
    x, high = where_ref[2], where_ref[3]
    own, mirror = spans(where_ref)
    rows, width = kv_ref.shape[1], kv_ref.shape[2] // 2
    dq_ref[...] = jnp.zeros_like(dq_ref)
    acc_ref[...] = jnp.zeros_like(acc_ref)
    for at in range(n):
        side, r = divmod(at, nx)
        cols = slice(at * rows, (at + 1) * rows)
        here = lax.rem(x - r + nx, nx)
        end = side ^ high
        maxima = [stat_ref[i, end, here, 0:1, :] for i in range(n)]
        top = functools.reduce(jnp.maximum, maxima)
        shares = [jnp.exp2(m - top) for m in maxima]
        total = sum(stat_ref[i, end, here, 1:2, :] * w for i, w in enumerate(shares))
        delta = sum(stat_ref[i, end, here, 2:3, :] * w for i, w in enumerate(shares))
        norm_ref[:, cols] = top + jnp.log2(total)
        delta_ref[:, cols] = delta / total
        share = jnp.exp2(mine_ref[end, here, 0:1, :] - top) / total
        out_refs[r][side * rows : (side + 1) * rows, width:] = jnp.transpose(
            o_ref[:, cols] * share
        ).astype(BF16)

    def unit(side, j, masked):
        k, v = kv_ref[j, :, :width], kv_ref[j, :, width:]
        dk = jnp.zeros((rows, width), F32)
        dv = jnp.zeros((rows, width), F32)
        for r in range(nx):
            at = side * nx + r
            cols = slice(at * rows, (at + 1) * rows)
            q, g = q_refs[at][:, :width], q_refs[at][:, width:]
            p = jnp.exp2(dot(k, q, NT) * rate - norm_ref[:, cols])
            if masked:
                p = jnp.where(allowed_pairs(rows, x, lax.rem(x - r + nx, nx)), p, 0.0)
            ds = (p * (dot(v, g, NT) - delta_ref[:, cols])).astype(BF16)
            dv = dv + dot(p.astype(BF16), g, NN)
            dk = dk + dot(ds, q, NN)
            dq_ref[:, cols] += dot(k, ds, TN)
        acc_ref[j, :, :width] += dk
        acc_ref[j, :, width:] += dv

    @pl.loop(0, own)
    def _(j):
        unit(0, j, False)

    unit(0, own, True)

    @pl.loop(0, mirror)
    def _(j):
        unit(1, j, False)

    dkv_ref[:, :, :width] = (acc_ref[:, :, :width] * scaling).astype(BF16)
    dkv_ref[:, :, width:] = acc_ref[:, :, width:].astype(BF16)
    for at in range(n):
        side, r = divmod(at, nx)
        cols = slice(at * rows, (at + 1) * rows)
        out_refs[r][side * rows : (side + 1) * rows, :width] = jnp.transpose(
            dq_ref[:, cols] * scaling
        ).astype(BF16)


def shifted(value, axis, count, step):
    return lax.ppermute(value, axis, [(i, (i + step) % count) for i in range(count)])


def mirrored(value, count):
    return lax.ppermute(value, Z, [(i, count - 1 - i) for i in range(count)])


def per_device(nj, nx, nh, queries, keys, values, out_grad):
    rows, width = queries.shape
    nz = 2 * nj
    scaling = 1.0 / math.sqrt(width)
    rate = scaling * math.log2(math.e)
    smem = pl.BlockSpec(memory_space=pltpu.SMEM)
    vmem = pl.BlockSpec(memory_space=pltpu.VMEM)
    own = jnp.concatenate([queries, out_grad], axis=1)
    other = mirrored(own, nz)
    blocks = [own] + [shifted(own, "x", nx, r) for r in range(1, nx)]
    blocks += [other] + [shifted(other, "x", nx, r) for r in range(1, nx)]
    mixed = jnp.concatenate(
        [keys.reshape(-1, nh, width), values.reshape(-1, nh, width)], axis=2
    ).transpose(1, 0, 2)
    kv = lax.all_to_all(
        jnp.broadcast_to(mixed, (nj, *mixed.shape)).reshape(nj * nh, *mixed.shape[1:]),
        ("zj", "head"), 0, 0, tiled=True,
    ).reshape(nj, rows, 2 * width)
    place = [lax.axis_index(a) for a in SEQ]
    where = jnp.stack([*place, place[0] * 2 // nj]).astype(jnp.int32)
    pairs = 5 * rows * nx * rows * width
    partial, mine = pl.pallas_call(
        functools.partial(forward_kernel, rate, nx),
        out_shape=(
            jax.ShapeDtypeStruct((width, 2 * nx * rows), F32),
            jax.ShapeDtypeStruct((2, nx, 8, rows), F32),
        ),
        in_specs=[smem] + [vmem] * (2 * nx + 1),
        out_specs=(vmem, vmem),
        scratch_shapes=[pltpu.VMEM((1, 2 * nx * rows), F32)] * 2,
        compiler_params=pltpu.CompilerParams(vmem_limit_bytes=VMEM),
        cost_estimate=pl.CostEstimate(flops=4 * pairs, bytes_accessed=2 << 20, transcendentals=0),
        name="forward",
    )(where, *blocks, kv)
    groups = [[z * nx + x for z in (m, nz - 1 - m) for x in range(nx)] for m in range(nj)]
    stats = lax.all_to_all(
        jnp.broadcast_to(mine, (2 * nx, *mine.shape)), SEQ, 0, 0,
        axis_index_groups=groups, tiled=True,
    )
    *parts, dkv = pl.pallas_call(
        functools.partial(backward_kernel, rate, scaling, nx),
        out_shape=(jax.ShapeDtypeStruct((2 * rows, 2 * width), BF16),) * nx
        + (jax.ShapeDtypeStruct(kv.shape, BF16),),
        in_specs=[smem] + [vmem] * (2 * nx + 4),
        out_specs=(vmem,) * (nx + 1),
        scratch_shapes=[
            pltpu.VMEM((width, 2 * nx * rows), F32),
            pltpu.VMEM((1, 2 * nx * rows), F32),
            pltpu.VMEM((1, 2 * nx * rows), F32),
            pltpu.VMEM(kv.shape, F32),
        ],
        compiler_params=pltpu.CompilerParams(vmem_limit_bytes=VMEM),
        cost_estimate=pl.CostEstimate(flops=10 * pairs, bytes_accessed=2 << 20, transcendentals=0),
        name="backward",
    )(where, *blocks, kv, partial, mine, stats)
    arrived = [shifted(parts[-r % nx], "x", nx, r) for r in range(1, nx)]
    total = functools.reduce(jnp.add, [a.astype(F32) for a in [parts[0], *arrived]])
    back = mirrored(total[rows:].astype(BF16), nz)
    dkv = lax.all_to_all(dkv, "zj", 0, 0, tiled=True)
    dkv = jnp.sum(dkv.astype(F32), axis=0)
    total = total[:rows] + back.astype(F32)
    return total[:, width:].astype(BF16), total[:, :width], dkv[:, :width], dkv[:, width:]


def solution(mesh):
    nh = mesh.shape["head"]
    split = Mesh(mesh.devices.reshape(4, 2, -1, nh), (*SEQ, "head"))
    return jax.shard_map(
        functools.partial(per_device, 4, split.shape["x"], nh),
        mesh=split,
        in_specs=(P(SEQ, "head"), P((*SEQ, "head"), None), P((*SEQ, "head"), None), P(SEQ, "head")),
        out_specs=(P(SEQ, "head"),) * 4,
        check_vma=False,
    )
```

```python
import functools
import math

import jax
import jax.numpy as jnp
from jax import lax
from jax.experimental import pallas as pl
from jax.experimental.pallas import tpu as pltpu
from jax.sharding import Mesh
from jax.sharding import PartitionSpec as P

Z = ("zj", "zp")
SEQ = (*Z, "x")
VMEM = 24 << 20
LOW = -1e30
F32 = jnp.float32
BF16 = jnp.bfloat16
NT = (((1,), (1,)), ((), ()))
TN = (((0,), (0,)), ((), ()))
NN = (((1,), (0,)), ((), ()))


def dot(a, b, dims):
    return lax.dot_general(a, b, dims, preferred_element_type=F32)


def allowed_pairs(rows, key_block, query_block):
    key_pos = lax.broadcasted_iota(jnp.int32, (rows, rows), 0) + key_block * rows
    query_pos = lax.broadcasted_iota(jnp.int32, (rows, rows), 1) + query_block * rows
    return key_pos <= query_pos


def spans(where_ref):
    zj, zp = where_ref[0], where_ref[1]
    return zj, 4 - zp - zj


def forward_kernel(rate, nx, where_ref, *refs):
    q_refs, (kv_ref, o_ref, stat_ref, m_ref, l_ref) = refs[: 2 * nx], refs[2 * nx :]
    x, high = where_ref[2], where_ref[3]
    own, mirror = spans(where_ref)
    rows, width = kv_ref.shape[1], kv_ref.shape[2] // 2
    m_ref[...] = jnp.full_like(m_ref, LOW)
    l_ref[...] = jnp.zeros_like(l_ref)
    o_ref[...] = jnp.zeros_like(o_ref)

    def unit(side, j, masked):
        k, v = kv_ref[j, :, :width], kv_ref[j, :, width:]
        for r in range(nx):
            at = side * nx + r
            cols = slice(at * rows, (at + 1) * rows)
            s = dot(k, q_refs[at][:, :width], NT)
            if masked:
                ok = allowed_pairs(rows, x, lax.rem(x - r + nx, nx))
                s = jnp.where(ok, s, LOW)
            m_old = m_ref[:, cols]
            m_new = jnp.maximum(m_old, jnp.max(s, axis=0, keepdims=True))
            p = jnp.exp2((s - m_new) * rate)
            if masked:
                p = jnp.where(ok, p, 0.0)
            alpha = jnp.exp2((m_old - m_new) * rate)
            m_ref[:, cols] = m_new
            l_ref[:, cols] = l_ref[:, cols] * alpha + jnp.sum(p, axis=0, keepdims=True)
            o_ref[:, cols] = o_ref[:, cols] * alpha + dot(v, p.astype(BF16), TN)

    @pl.loop(0, own)
    def _(j):
        unit(0, j, False)

    unit(0, own, True)

    @pl.loop(0, mirror)
    def _(j):
        unit(1, j, False)

    for at in range(2 * nx):
        side, r = divmod(at, nx)
        cols = slice(at * rows, (at + 1) * rows)
        grads = jnp.transpose(q_refs[at][:, width:].astype(F32))
        to = lax.rem(x - r + nx, nx)
        row = pl.ds((side ^ high) * nx + to, 1)
        stat_ref[0, row, :] = m_ref[:, cols] * rate
        stat_ref[1, row, :] = l_ref[:, cols]
        stat_ref[2, row, :] = jnp.sum(grads * o_ref[:, cols], axis=0, keepdims=True)


def backward_kernel(rate, scaling, nx, where_ref, *refs):
    n = 2 * nx
    q_refs, (kv_ref, o_ref, mine_ref, stat_ref), refs = refs[:n], refs[n : n + 4], refs[n + 4 :]
    out_refs, (dkv_ref, dq_ref, norm_ref, delta_ref, acc_ref) = refs[:nx], refs[nx:]
    x, high = where_ref[2], where_ref[3]
    own, mirror = spans(where_ref)
    rows, width = kv_ref.shape[1], kv_ref.shape[2] // 2
    dq_ref[...] = jnp.zeros_like(dq_ref)
    acc_ref[...] = jnp.zeros_like(acc_ref)
    for at in range(n):
        side, r = divmod(at, nx)
        cols = slice(at * rows, (at + 1) * rows)
        here = lax.rem(x - r + nx, nx)
        row = pl.ds((side ^ high) * nx + here, 1)
        maxima = [stat_ref[i, 0, row, :] for i in range(n)]
        top = functools.reduce(jnp.maximum, maxima)
        shares = [jnp.exp2(m - top) for m in maxima]
        total = sum(stat_ref[i, 1, row, :] * w for i, w in enumerate(shares))
        delta = sum(stat_ref[i, 2, row, :] * w for i, w in enumerate(shares))
        norm_ref[:, cols] = top + jnp.log2(total)
        delta_ref[:, cols] = delta / total
        share = jnp.exp2(mine_ref[0, row, :] - top) / total
        out_refs[r][side * rows : (side + 1) * rows, width:] = jnp.transpose(
            o_ref[:, cols] * share
        ).astype(BF16)

    def unit(side, j, masked):
        k, v = kv_ref[j, :, :width], kv_ref[j, :, width:]
        dk = jnp.zeros((rows, width), F32)
        dv = jnp.zeros((rows, width), F32)
        for r in range(nx):
            at = side * nx + r
            cols = slice(at * rows, (at + 1) * rows)
            q, g = q_refs[at][:, :width], q_refs[at][:, width:]
            p = jnp.exp2(dot(k, q, NT) * rate - norm_ref[:, cols])
            if masked:
                p = jnp.where(allowed_pairs(rows, x, lax.rem(x - r + nx, nx)), p, 0.0)
            ds = (p * (dot(v, g, NT) - delta_ref[:, cols])).astype(BF16)
            dv = dv + dot(p.astype(BF16), g, NN)
            dk = dk + dot(ds, q, NN)
            dq_ref[:, cols] += dot(k, ds, TN)
        acc_ref[j, :, :width] += dk
        acc_ref[j, :, width:] += dv

    @pl.loop(0, own)
    def _(j):
        unit(0, j, False)

    unit(0, own, True)

    @pl.loop(0, mirror)
    def _(j):
        unit(1, j, False)

    dkv_ref[:, :, :width] = (acc_ref[:, :, :width] * scaling).astype(BF16)
    dkv_ref[:, :, width:] = acc_ref[:, :, width:].astype(BF16)
    for at in range(n):
        side, r = divmod(at, nx)
        cols = slice(at * rows, (at + 1) * rows)
        out_refs[r][side * rows : (side + 1) * rows, :width] = jnp.transpose(
            dq_ref[:, cols] * scaling
        ).astype(BF16)


def shifted(value, axis, count, step):
    return lax.ppermute(value, axis, [(i, (i + step) % count) for i in range(count)])


def mirrored(value, count):
    return lax.ppermute(value, Z, [(i, count - 1 - i) for i in range(count)])


def per_device(nj, nx, nh, queries, keys, values, out_grad):
    rows, width = queries.shape
    nz = 2 * nj
    scaling = 1.0 / math.sqrt(width)
    rate = scaling * math.log2(math.e)
    smem = pl.BlockSpec(memory_space=pltpu.SMEM)
    vmem = pl.BlockSpec(memory_space=pltpu.VMEM)
    own = jnp.concatenate([queries, out_grad], axis=1)
    other = mirrored(own, nz)
    blocks = [own] + [shifted(own, "x", nx, r) for r in range(1, nx)]
    blocks += [other] + [shifted(other, "x", nx, r) for r in range(1, nx)]
    mixed = jnp.concatenate(
        [keys.reshape(-1, nh, width), values.reshape(-1, nh, width)], axis=2
    ).transpose(1, 0, 2)
    mixed = jnp.broadcast_to(mixed, (nj, *mixed.shape)).reshape(nj * nh, *mixed.shape[1:])
    kv = lax.all_to_all(mixed, ("zj", "head"), 0, 0, tiled=True)
    kv = kv.reshape(nj, rows, 2 * width)
    place = [lax.axis_index(a) for a in SEQ]
    where = jnp.stack([*place, place[0] * 2 // nj]).astype(jnp.int32)
    pairs = 5 * rows * nx * rows * width
    partial, mine = pl.pallas_call(
        functools.partial(forward_kernel, rate, nx),
        out_shape=(
            jax.ShapeDtypeStruct((width, 2 * nx * rows), F32),
            jax.ShapeDtypeStruct((3, 2 * nx, rows), F32),
        ),
        in_specs=[smem] + [vmem] * (2 * nx + 1),
        out_specs=(vmem, vmem),
        scratch_shapes=[pltpu.VMEM((1, 2 * nx * rows), F32)] * 2,
        compiler_params=pltpu.CompilerParams(vmem_limit_bytes=VMEM),
        cost_estimate=pl.CostEstimate(flops=4 * pairs, bytes_accessed=2 << 20, transcendentals=0),
        name="forward",
    )(where, *blocks, kv)
    groups = [[z * nx + x for z in (m, nz - 1 - m) for x in range(nx)] for m in range(nj)]
    stats = lax.all_to_all(
        jnp.broadcast_to(mine, (2 * nx, *mine.shape)), SEQ, 0, 0,
        axis_index_groups=groups, tiled=True,
    )
    *parts, dkv = pl.pallas_call(
        functools.partial(backward_kernel, rate, scaling, nx),
        out_shape=(jax.ShapeDtypeStruct((2 * rows, 2 * width), BF16),) * nx
        + (jax.ShapeDtypeStruct(kv.shape, BF16),),
        in_specs=[smem] + [vmem] * (2 * nx + 4),
        out_specs=(vmem,) * (nx + 1),
        scratch_shapes=[
            pltpu.VMEM((width, 2 * nx * rows), F32),
            pltpu.VMEM((1, 2 * nx * rows), F32),
            pltpu.VMEM((1, 2 * nx * rows), F32),
            pltpu.VMEM(kv.shape, F32),
        ],
        compiler_params=pltpu.CompilerParams(vmem_limit_bytes=VMEM),
        cost_estimate=pl.CostEstimate(flops=10 * pairs, bytes_accessed=2 << 20, transcendentals=0),
        name="backward",
    )(where, *blocks, kv, partial, mine, stats)
    arrived = [shifted(parts[-r % nx], "x", nx, r) for r in range(1, nx)]
    total = functools.reduce(jnp.add, [a.astype(F32) for a in [parts[0], *arrived]])
    back = mirrored(total[rows:].astype(BF16), nz)
    dkv = lax.all_to_all(dkv, "zj", 0, 0, tiled=True)
    dkv = jnp.sum(dkv.astype(F32), axis=0)
    total = total[:rows] + back.astype(F32)
    return total[:, width:].astype(BF16), total[:, :width], dkv[:, :width], dkv[:, width:]


def solution(mesh):
    nh = mesh.shape["head"]
    split = Mesh(mesh.devices.reshape(4, 2, -1, nh), (*SEQ, "head"))
    return jax.shard_map(
        functools.partial(per_device, 4, split.shape["x"], nh),
        mesh=split,
        in_specs=(P(SEQ, "head"), P((*SEQ, "head"), None), P((*SEQ, "head"), None), P(SEQ, "head")),
        out_specs=(P(SEQ, "head"),) * 4,
        check_vma=False,
    )
```

```python
import functools
import math

import jax
import jax.numpy as jnp
from jax import lax
from jax.experimental import pallas as pl
from jax.experimental.pallas import tpu as pltpu
from jax.sharding import Mesh
from jax.sharding import PartitionSpec as P

Z = ("zj", "zp")
SEQ = (*Z, "x")
VMEM = 24 << 20
PIECES = (3, 2, 2)
LOW = -1e30
F32 = jnp.float32
BF16 = jnp.bfloat16
NT = (((1,), (1,)), ((), ()))
TN = (((0,), (0,)), ((), ()))
NN = (((1,), (0,)), ((), ()))


def dot(a, b, dims):
    return lax.dot_general(a, b, dims, preferred_element_type=F32)


def allowed_pairs(rows, key_block, query_block):
    key_pos = lax.broadcasted_iota(jnp.int32, (rows, rows), 0) + key_block * rows
    query_pos = lax.broadcasted_iota(jnp.int32, (rows, rows), 1) + query_block * rows
    return key_pos <= query_pos


def prepare_kernel(nh, q_ref, g_ref, k_ref, v_ref, own_ref, mixed_ref, kv_ref, sems):
    width = q_ref.shape[1]
    moves = [
        pltpu.make_async_copy(k_ref, kv_ref.at[0], sems.at[0]),
        pltpu.make_async_copy(v_ref, kv_ref.at[1], sems.at[1]),
        pltpu.make_async_copy(q_ref, own_ref.at[:, :width], sems.at[2]),
        pltpu.make_async_copy(g_ref, own_ref.at[:, width:], sems.at[3]),
    ]
    for move in moves:
        move.start()
    for part in range(2):
        moves[part].wait()
        for at in range(mixed_ref.shape[0]):
            cols = slice(at % nh * width, (at % nh + 1) * width)
            mixed_ref[at, :, part * width : (part + 1) * width] = kv_ref[part, :, cols]
    moves[2].wait()
    moves[3].wait()


def pieces(value, count):
    out = []
    for _ in range(count):
        out.append(value.astype(BF16))
        value = value - out[-1].astype(F32)
    return out


def gather_blocks(q_refs, query_ref, grad_ref):
    rows, width = q_refs[0].shape[0], q_refs[0].shape[1] // 2
    count = len(q_refs) // 2
    for at, ref in enumerate(q_refs):
        side, r = divmod(at, count)
        query_ref[side, r * rows : (r + 1) * rows, :] = ref[:, :width]
        grad_ref[side, r * rows : (r + 1) * rows, :] = ref[:, width:]


def each_unit(where_ref, unit):
    own, other = where_ref[0], where_ref[1]

    @pl.loop(0, own)
    def _(j):
        unit(j, 0, j, False)

    unit(own, 0, own, True)

    @pl.loop(0, other)
    def _(j):
        unit(own + 1 + j, 1, j, False)


def folded(value, op):
    return op(value.reshape(value.shape[0] // 8, 8, value.shape[1]), axis=0)


def forward_kernel(rate, nx, where_ref, *refs):
    q_refs, (kv_ref, send_ref, s_ref), refs = refs[: 2 * nx], refs[2 * nx : 2 * nx + 3], refs[2 * nx + 3 :]
    stat_ref, o_ref, m_ref, l_ref, query_ref, grad_ref = refs
    x, even = where_ref[2], where_ref[3]
    rows, width = kv_ref.shape[1], kv_ref.shape[2] // 2
    gather_blocks(q_refs, query_ref, grad_ref)
    m_ref[...] = jnp.full_like(m_ref, LOW)
    l_ref[...] = jnp.zeros_like(l_ref)
    o_ref[...] = jnp.zeros_like(o_ref)

    def score(u, side, j, masked):
        s = dot(kv_ref[j, :, :width], query_ref[side], NT)
        if masked:
            oks = [allowed_pairs(rows, x, lax.rem(x - r + nx, nx)) for r in range(nx)]
            s = jnp.where(jnp.concatenate(oks, axis=1), s, LOW)
        s_ref[u] = s
        m_ref[side] = jnp.maximum(m_ref[side], folded(s, jnp.max))

    def weigh(u, side, j, masked):
        p = jnp.exp2((s_ref[u] - m_ref[side, 0:1, :]) * rate)
        l_ref[side] += folded(p, jnp.sum)
        o_ref[side] += dot(kv_ref[j, :, width:], p.astype(BF16), TN)

    each_unit(where_ref, score)
    for side in range(2):
        m_ref[side, 0:1, :] = jnp.maximum(
            jnp.max(m_ref[side], axis=0, keepdims=True), LOW / 2
        )
    each_unit(where_ref, weigh)
    for side in range(2):
        total = jnp.sum(l_ref[side], axis=0, keepdims=True)
        grads = jnp.transpose(grad_ref[side].astype(F32))
        inner = jnp.sum(grads * o_ref[side], axis=0, keepdims=True)
        for r in range(nx):
            cols = slice(r * rows, (r + 1) * rows)
            to = (side ^ even) * nx + lax.rem(x - r + nx, nx)
            row = pl.ds(to, 1)
            stat_ref[0, row, :] = m_ref[side, 0:1, cols] * rate
            stat_ref[1, row, :] = total[:, cols]
            stat_ref[2, row, :] = inner[:, cols]
            send_ref[to, :width, :] = o_ref[side, :, cols].astype(BF16)
    base = width
    for q, count in enumerate(PIECES):
        for piece in pieces(stat_ref[q], count):
            for to in range(2 * nx):
                send_ref[to, base : base + 2 * nx, :] = piece
            base += 2 * nx


def read_stats(got_ref, stat_ref, base, n):
    for q, count in enumerate(PIECES):
        for i in range(n):
            stat_ref[i, q] = sum(
                got_ref[i, base + c * n : base + (c + 1) * n, :].astype(F32) for c in range(count)
            )
        base += count * n


def backward_kernel(rate, scaling, nx, where_ref, *refs):
    n = 2 * nx
    q_refs, (kv_ref, got_ref, s_ref), refs = refs[:n], refs[n : n + 3], refs[n + 3 :]
    nj = kv_ref.shape[0]
    out_refs, key_refs, refs = refs[:nx], refs[nx : nx + nj], refs[nx + nj :]
    dq_ref, norm_ref, delta_ref, acc_ref, stat_ref, query_ref, grad_ref = refs
    x, even = where_ref[2], where_ref[3]
    rows, width = kv_ref.shape[1], kv_ref.shape[2] // 2
    read_stats(got_ref, stat_ref, width, n)
    gather_blocks(q_refs, query_ref, grad_ref)
    dq_ref[...] = jnp.zeros_like(dq_ref)
    acc_ref[...] = jnp.zeros_like(acc_ref)
    top = functools.reduce(jnp.maximum, [stat_ref[i, 0] for i in range(n)])
    shares = [jnp.exp2(stat_ref[i, 0] - top) for i in range(n)]
    total = sum(stat_ref[i, 1] * w for i, w in enumerate(shares))
    delta = sum(stat_ref[i, 2] * w for i, w in enumerate(shares))
    stat_ref[0, 0] = top + jnp.log2(total)
    stat_ref[0, 1] = delta / total
    for at in range(n):
        side, r = divmod(at, nx)
        cols = slice(r * rows, (r + 1) * rows)
        row = pl.ds((side ^ even) * nx + lax.rem(x - r + nx, nx), 1)
        norm_ref[side, :, cols] = stat_ref[0, 0, row, :]
        delta_ref[side, :, cols] = stat_ref[0, 1, row, :]

    def unit(u, side, j, masked):
        k, v = kv_ref[j, :, :width], kv_ref[j, :, width:]
        p = jnp.exp2(s_ref[u] * rate - norm_ref[side])
        ds = (p * (dot(v, grad_ref[side], NT) - delta_ref[side])).astype(BF16)
        acc_ref[j, :, width:] += dot(p.astype(BF16), grad_ref[side], NN)
        acc_ref[j, :, :width] += dot(ds, query_ref[side], NN)
        dq_ref[side] += dot(k, ds, TN)

    each_unit(where_ref, unit)
    for step in range(nj):
        to = lax.rem(where_ref[0] + step, nj)
        key_refs[step][:, :width] = (acc_ref[to, :, :width] * scaling).astype(BF16)
        key_refs[step][:, width:] = acc_ref[to, :, width:].astype(BF16)
    for at in range(n):
        side, r = divmod(at, nx)
        out_refs[r][:, side * rows : (side + 1) * rows] = (
            dq_ref[side, :, r * rows : (r + 1) * rows] * scaling
        ).astype(BF16)


def mix_kernel(nx, where_ref, got_ref, out_ref, stat_ref):
    n = 2 * nx
    rows, width = out_ref.shape
    read_stats(got_ref, stat_ref, width, n)
    row = pl.ds(where_ref[3] * nx + where_ref[2], 1)
    maxima = [stat_ref[i, 0, row, :] for i in range(n)]
    top = functools.reduce(jnp.maximum, maxima)
    shares = [jnp.exp2(m - top) for m in maxima]
    total = sum(stat_ref[i, 1, row, :] * w for i, w in enumerate(shares))
    mixed = jnp.zeros((width, rows), F32)
    for i, share in enumerate(shares):
        mixed = mixed + share * got_ref[i, :width, :]
    out_ref[...] = jnp.transpose(mixed / total).astype(BF16)


def final_kernel(nx, nj, *refs):
    part_refs, back_ref, key_refs, outs = refs[:nx], refs[nx], refs[nx + 1 : -3], refs[-3:]
    rows, width = outs[0].shape
    dq = back_ref[...].astype(F32)
    for part in part_refs:
        dq = dq + part[:, :rows]
    outs[0][...] = jnp.transpose(dq)
    total = key_refs[0][...].astype(F32)
    for j in range(1, nj):
        total = total + key_refs[j][...]
    outs[1][...] = total[:, :width]
    outs[2][...] = total[:, width:]


def shifted(value, axis, count, step):
    return lax.ppermute(value, axis, [(i, (i + step) % count) for i in range(count)])


def swapped(value, count):
    pairs = [(i, (i + 1) % count) for i in range(1, count, 2)]
    return lax.ppermute(value, Z, pairs + [(j, i) for i, j in pairs])


def per_device(nj, nx, nh, queries, keys, values, out_grad):
    rows, width = queries.shape
    nz = 2 * nj
    scaling = 1.0 / math.sqrt(width)
    rate = scaling * math.log2(math.e)
    smem = pl.BlockSpec(memory_space=pltpu.SMEM)
    vmem = pl.BlockSpec(memory_space=pltpu.VMEM)
    own, mixed = pl.pallas_call(
        functools.partial(prepare_kernel, nh),
        out_shape=(
            jax.ShapeDtypeStruct((rows, 2 * width), BF16),
            jax.ShapeDtypeStruct((nj * nh, keys.shape[0], 2 * width), BF16),
        ),
        in_specs=[pl.BlockSpec(memory_space=pltpu.HBM)] * 4,
        out_specs=(vmem,) * 2,
        scratch_shapes=[pltpu.VMEM((2, *keys.shape), BF16), pltpu.SemaphoreType.DMA((4,))],
        compiler_params=pltpu.CompilerParams(vmem_limit_bytes=60 << 20),
        name="prepare",
    )(queries, out_grad, keys, values)
    other_own = swapped(own, nz)
    blocks = [own, shifted(own, "x", nx, 1)]
    blocks += [shifted(own, "x", nx, r) for r in range(2, nx)]
    blocks += [other_own] + [shifted(other_own, "x", nx, r) for r in range(1, nx)]
    kv = lax.all_to_all(mixed, ("zj", "head"), 0, 0, tiled=True)
    kv = kv.reshape(nj, rows, 2 * width)
    zj, zp, x = (lax.axis_index(a) for a in SEQ)
    other = jnp.where(zp == 0, jnp.where(zj == 0, nj, zj), lax.rem(zj + 1, nj))
    where = jnp.stack([zj, other, x, 1 - zp]).astype(jnp.int32)
    pairs = 7 * rows * nx * rows * width
    sent = (2 * nx, width + sum(PIECES) * 2 * nx, rows)
    units = (2 * nj - 1, rows, nx * rows)
    stat = pltpu.VMEM((2 * nx, len(PIECES), 2 * nx, rows), F32)
    gathered = [pltpu.VMEM((2, nx * rows, width), BF16)] * 2
    parts, scores = pl.pallas_call(
        functools.partial(forward_kernel, rate, nx),
        out_shape=(jax.ShapeDtypeStruct(sent, BF16), jax.ShapeDtypeStruct(units, F32)),
        in_specs=[smem] + [vmem] * (2 * nx + 1),
        out_specs=(vmem, vmem),
        scratch_shapes=[
            pltpu.VMEM((len(PIECES), 2 * nx, rows), F32),
            pltpu.VMEM((2, width, nx * rows), F32),
            pltpu.VMEM((2, 8, nx * rows), F32),
            pltpu.VMEM((2, 8, nx * rows), F32),
            *gathered,
        ],
        compiler_params=pltpu.CompilerParams(vmem_limit_bytes=VMEM),
        cost_estimate=pl.CostEstimate(flops=4 * pairs, bytes_accessed=2 << 20, transcendentals=0),
        name="forward",
    )(where, *blocks, kv)
    groups = [[z * nx + i for z in (m, (m + 1) % nz) for i in range(nx)] for m in range(1, nz, 2)]
    got = lax.all_to_all(parts, SEQ, 0, 0, axis_index_groups=groups, tiled=True)
    both = pl.pallas_call(
        functools.partial(backward_kernel, rate, scaling, nx),
        out_shape=(jax.ShapeDtypeStruct((width, 2 * rows), BF16),) * nx
        + (jax.ShapeDtypeStruct((rows, 2 * width), BF16),) * nj,
        in_specs=[smem] + [vmem] * (2 * nx + 3),
        out_specs=(vmem,) * (nx + nj),
        scratch_shapes=[
            pltpu.VMEM((2, width, nx * rows), F32),
            pltpu.VMEM((2, 1, nx * rows), F32),
            pltpu.VMEM((2, 1, nx * rows), F32),
            pltpu.VMEM(kv.shape, F32),
            stat,
            *gathered,
        ],
        compiler_params=pltpu.CompilerParams(vmem_limit_bytes=VMEM),
        cost_estimate=pl.CostEstimate(flops=10 * pairs, bytes_accessed=2 << 20, transcendentals=0),
        name="backward",
    )(where, *blocks, kv, got, scores)
    parts, dkv = both[:nx], both[nx:]
    parts = [parts[0]] + [shifted(parts[-r % nx], "x", nx, r) for r in range(1, nx)]
    dkv = [dkv[0]] + [shifted(dkv[r], "zj", nj, r) for r in range(1, nj)]
    attended = pl.pallas_call(
        functools.partial(mix_kernel, nx),
        out_shape=jax.ShapeDtypeStruct((rows, width), BF16),
        in_specs=[smem, vmem],
        out_specs=vmem,
        scratch_shapes=[stat],
        compiler_params=pltpu.CompilerParams(vmem_limit_bytes=8 << 20),
        name="mix",
    )(where, got)
    back = functools.reduce(jnp.add, [p[:, rows:].astype(F32) for p in parts])
    back = swapped(back.astype(BF16), nz)
    sums = pl.pallas_call(
        functools.partial(final_kernel, nx, nj),
        out_shape=(jax.ShapeDtypeStruct((rows, width), F32),) * 3,
        in_specs=[vmem] * (nx + nj + 1),
        out_specs=(vmem,) * 3,
        compiler_params=pltpu.CompilerParams(vmem_limit_bytes=8 << 20),
        name="final",
    )(*parts, back, *dkv)
    return attended, *sums


def solution(mesh):
    nh = mesh.shape["head"]
    split = Mesh(mesh.devices.reshape(4, 2, -1, nh), (*SEQ, "head"))
    return jax.shard_map(
        functools.partial(per_device, 4, split.shape["x"], nh),
        mesh=split,
        in_specs=(P(SEQ, "head"), P((*SEQ, "head"), None), P((*SEQ, "head"), None), P(SEQ, "head")),
        out_specs=(P(SEQ, "head"),) * 4,
        check_vma=False,
    )
```

```python
import functools
import math

import jax
import jax.numpy as jnp
from jax import lax
from jax.experimental import pallas as pl
from jax.experimental.pallas import tpu as pltpu
from jax.sharding import Mesh
from jax.sharding import PartitionSpec as P

Z = ("zj", "zp")
SEQ = (*Z, "x")
VMEM = 24 << 20
LOW = -1e30
F32 = jnp.float32
BF16 = jnp.bfloat16
NT = (((1,), (1,)), ((), ()))
TN = (((0,), (0,)), ((), ()))
NN = (((1,), (0,)), ((), ()))


def dot(a, b, dims):
    return lax.dot_general(a, b, dims, preferred_element_type=F32)


def allowed_pairs(rows, key_block, query_block):
    key_pos = lax.broadcasted_iota(jnp.int32, (rows, rows), 0) + key_block * rows
    query_pos = lax.broadcasted_iota(jnp.int32, (rows, rows), 1) + query_block * rows
    return key_pos <= query_pos


def diagonal(rows, x, nx):
    oks = [allowed_pairs(rows, x, lax.rem(x - r + nx, nx)) for r in range(nx)]
    return jnp.concatenate(oks, axis=1)


def prepare_kernel(nh, q_ref, g_ref, k_ref, v_ref, own_ref, mixed_ref, kv_ref, sems):
    width = q_ref.shape[1]
    moves = [
        pltpu.make_async_copy(k_ref, kv_ref.at[0], sems.at[0]),
        pltpu.make_async_copy(v_ref, kv_ref.at[1], sems.at[1]),
        pltpu.make_async_copy(q_ref, own_ref.at[:, :width], sems.at[2]),
        pltpu.make_async_copy(g_ref, own_ref.at[:, width:], sems.at[3]),
    ]
    for move in moves:
        move.start()
    for part in range(2):
        moves[part].wait()
        for at in range(mixed_ref.shape[0]):
            cols = slice(at % nh * width, (at % nh + 1) * width)
            mixed_ref[at, :, part * width : (part + 1) * width] = kv_ref[part, :, cols]
    moves[2].wait()
    moves[3].wait()


def gather_blocks(q_refs, query_ref, grad_ref):
    rows, width = q_refs[0].shape[0], q_refs[0].shape[1] // 2
    count = (len(q_refs) + 1) // 2
    for at, ref in enumerate(q_refs, 1):
        side, r = divmod(at, count)
        query_ref[side, r * rows : (r + 1) * rows, :] = ref[:, :width]
        grad_ref[side, r * rows : (r + 1) * rows, :] = ref[:, width:]


def each_unit(where_ref, last, unit):
    own, full = where_ref[0], where_ref[0] + where_ref[1]

    def whole(f, lane):
        side = jnp.where(f >= own, 1, 0)
        unit(f, side, f - side * own, False, lane)

    @pl.loop(0, full // 2)
    def _(i):
        whole(2 * i, 0)
        whole(2 * i + 1, 1)

    @pl.when(full % 2 == 1)
    def _():
        whole(full - 1, 0)
        unit(last, 0, own, True, 1)

    @pl.when(full % 2 == 0)
    def _():
        unit(last, 0, own, True, 0)


def folded(value, op):
    return op(value.reshape(value.shape[0] // 8, 8, value.shape[1]), axis=0)


def forward_kernel(rate, nx, where_ref, *refs):
    n = 2 * nx
    (own_q_ref, own_g_ref), q_refs, kv_ref, refs = refs[:2], refs[2 : n + 1], refs[n + 1], refs[n + 2 :]
    out_refs, (send_ref, query_ref, grad_ref), refs = refs[:nx], refs[nx : nx + 3], refs[nx + 3 :]
    s_ref, stat_ref, o_ref, m_ref, l_ref, sems = refs
    x, even = where_ref[2], where_ref[3]
    rows, width = kv_ref.shape[1], kv_ref.shape[2] // 2
    moves = [
        pltpu.make_async_copy(own_q_ref, query_ref.at[0, :rows, :], sems.at[0]),
        pltpu.make_async_copy(own_g_ref, grad_ref.at[0, :rows, :], sems.at[1]),
    ]
    for move in moves:
        move.start()
    gather_blocks(q_refs, query_ref, grad_ref)
    m_ref[...] = jnp.full_like(m_ref, LOW)
    l_ref[...] = jnp.zeros_like(l_ref)
    o_ref[...] = jnp.zeros_like(o_ref)
    for move in moves:
        move.wait()

    def score(u, side, j, masked, lane):
        s = dot(kv_ref[j, :, :width], query_ref[side], NT)
        if masked:
            s = jnp.where(diagonal(rows, x, nx), s, LOW)
        s_ref[u] = s
        m_ref[lane, side] = jnp.maximum(m_ref[lane, side], folded(s, jnp.max))

    def weigh(u, side, j, masked, lane):
        p = jnp.exp2((s_ref[u] - m_ref[0, side, 0:1, :]) * rate)
        l_ref[lane, side] += folded(p, jnp.sum)
        o_ref[lane, side] += dot(kv_ref[j, :, width:], p.astype(BF16), TN)

    last = s_ref.shape[0] - 1
    each_unit(where_ref, last, score)
    for side in range(2):
        both = jnp.maximum(m_ref[0, side], m_ref[1, side])
        m_ref[0, side, 0:1, :] = jnp.maximum(jnp.max(both, axis=0, keepdims=True), LOW / 2)
    each_unit(where_ref, last, weigh)
    for side in range(2):
        total = jnp.sum(l_ref[0, side] + l_ref[1, side], axis=0, keepdims=True)
        o_ref[0, side] += o_ref[1, side]
        grads = jnp.transpose(grad_ref[side].astype(F32))
        inner = jnp.sum(grads * o_ref[0, side], axis=0, keepdims=True)
        for r in range(nx):
            cols = slice(r * rows, (r + 1) * rows)
            at = (side ^ even) * nx + lax.rem(x - r + nx, nx)
            stat_ref[pl.ds(at, 1), :] = m_ref[0, side, 0:1, cols] * rate
            stat_ref[pl.ds(n + at, 1), :] = total[:, cols]
            stat_ref[pl.ds(2 * n + at, 1), :] = inner[:, cols]
            out_refs[r][:, side * rows : (side + 1) * rows] = o_ref[0, side, :, cols].astype(BF16)
    for to in range(n):
        send_ref[to] = stat_ref[...]


def backward_kernel(rate, scaling, nx, where_ref, *refs):
    n = 2 * nx
    (query_ref, grad_ref, kv_ref, got_ref), refs = refs[:4], refs[4:]
    nj = kv_ref.shape[0]
    out_refs, key_refs, refs = refs[:nx], refs[nx : nx + nj], refs[nx + nj :]
    dq_ref, norm_ref, delta_ref, acc_ref, row_ref = refs
    x, even = where_ref[2], where_ref[3]
    rows, width = kv_ref.shape[1], kv_ref.shape[2] // 2
    dq_ref[...] = jnp.zeros_like(dq_ref)
    acc_ref[...] = jnp.zeros_like(acc_ref)
    maxima = [got_ref[i, :n] for i in range(n)]
    top = functools.reduce(jnp.maximum, maxima)
    shares = [jnp.exp2(m - top) for m in maxima]
    total = sum(got_ref[i, n : 2 * n] * w for i, w in enumerate(shares))
    delta = sum(got_ref[i, 2 * n :] * w for i, w in enumerate(shares))
    row_ref[0] = top + jnp.log2(total)
    row_ref[1] = delta / total
    for at in range(n):
        side, r = divmod(at, nx)
        cols = slice(r * rows, (r + 1) * rows)
        row = pl.ds((side ^ even) * nx + lax.rem(x - r + nx, nx), 1)
        norm_ref[side, :, cols] = row_ref[0, row, :]
        delta_ref[side, :, cols] = row_ref[1, row, :]

    def unit(u, side, j, masked, lane):
        k, v = kv_ref[j, :, :width], kv_ref[j, :, width:]
        s = dot(k, query_ref[side], NT)
        if masked:
            s = jnp.where(diagonal(rows, x, nx), s, LOW)
        p = jnp.exp2(s * rate - norm_ref[side])
        ds = (p * (dot(v, grad_ref[side], NT) - delta_ref[side])).astype(BF16)
        acc_ref[lane, j, :, width:] += dot(p.astype(BF16), grad_ref[side], NN)
        acc_ref[lane, j, :, :width] += dot(ds, query_ref[side], NN)
        dq_ref[lane, side] += dot(k, ds, TN)

    each_unit(where_ref, 0, unit)
    for step in range(nj):
        to = lax.rem(where_ref[0] + step, nj)
        both = acc_ref[0, to] + acc_ref[1, to]
        key_refs[step][:, :width] = (both[:, :width] * scaling).astype(BF16)
        key_refs[step][:, width:] = both[:, width:].astype(BF16)
    for at in range(n):
        side, r = divmod(at, nx)
        cols = slice(r * rows, (r + 1) * rows)
        out_refs[r][:, side * rows : (side + 1) * rows] = (
            (dq_ref[0, side, :, cols] + dq_ref[1, side, :, cols]) * scaling
        ).astype(BF16)


def mix_kernel(nx, where_ref, got_ref, *refs):
    part_refs, outs = refs[:nx], refs[nx:]
    x, even = where_ref[2], where_ref[3]
    n = 2 * nx
    width, rows = part_refs[0].shape[0], part_refs[0].shape[1] // 2
    for side in range(2):
        at = (side ^ even) * nx + x
        maxima = [got_ref[i, pl.ds(at, 1), :] for i in range(n)]
        top = functools.reduce(jnp.maximum, maxima)
        sums = [got_ref[i, pl.ds(n + at, 1), :] * jnp.exp2(m - top) for i, m in enumerate(maxima)]
        total = sum(sums)
        mixed = jnp.zeros((width, rows), F32)
        for e in range(nx):
            peer = even * nx + lax.rem(x - e + nx, nx)
            share = jnp.exp2(got_ref[peer, pl.ds(at, 1), :] - top) / total
            mixed = mixed + share * part_refs[e][:, side * rows : (side + 1) * rows]
        outs[side][...] = mixed.astype(outs[side].dtype)


def final_kernel(nx, nj, *refs):
    part_refs, (near_ref, back_ref), key_refs, outs = refs[:nx], refs[nx : nx + 2], refs[nx + 2 : -4], refs[-4:]
    rows, width = outs[0].shape
    dq = back_ref[:, :rows].astype(F32)
    for part in part_refs:
        dq = dq + part[:, :rows]
    outs[0][...] = jnp.transpose(near_ref[...] + back_ref[:, rows:]).astype(BF16)
    outs[1][...] = jnp.transpose(dq)
    total = key_refs[0][...].astype(F32)
    for j in range(1, nj):
        total = total + key_refs[j][...]
    outs[2][...] = total[:, :width]
    outs[3][...] = total[:, width:]


def shifted(value, axis, count, step):
    return lax.ppermute(value, axis, [(i, (i + step) % count) for i in range(count)])


def swapped(value, count):
    pairs = [(i, (i + 1) % count) for i in range(1, count, 2)]
    return lax.ppermute(value, Z, pairs + [(j, i) for i, j in pairs])


def per_device(nj, nx, nh, queries, keys, values, out_grad):
    rows, width = queries.shape
    nz = 2 * nj
    scaling = 1.0 / math.sqrt(width)
    rate = scaling * math.log2(math.e)
    smem = pl.BlockSpec(memory_space=pltpu.SMEM)
    vmem = pl.BlockSpec(memory_space=pltpu.VMEM)
    own, mixed = pl.pallas_call(
        functools.partial(prepare_kernel, nh),
        out_shape=(
            jax.ShapeDtypeStruct((rows, 2 * width), BF16),
            jax.ShapeDtypeStruct((nj * nh, keys.shape[0], 2 * width), BF16),
        ),
        in_specs=[pl.BlockSpec(memory_space=pltpu.HBM)] * 4,
        out_specs=(vmem,) * 2,
        scratch_shapes=[pltpu.VMEM((2, *keys.shape), BF16), pltpu.SemaphoreType.DMA((4,))],
        compiler_params=pltpu.CompilerParams(vmem_limit_bytes=60 << 20),
        name="prepare",
    )(queries, out_grad, keys, values)
    other_own = swapped(own, nz)
    blocks = [own, shifted(own, "x", nx, 1)]
    blocks += [shifted(own, "x", nx, r) for r in range(2, nx)]
    blocks += [other_own] + [shifted(other_own, "x", nx, r) for r in range(1, nx)]
    kv = lax.all_to_all(mixed, ("zj", "head"), 0, 0, tiled=True)
    kv = kv.reshape(nj, rows, 2 * width)
    zj, zp, x = (lax.axis_index(a) for a in SEQ)
    other = jnp.where(zp == 0, jnp.where(zj == 0, nj, zj), lax.rem(zj + 1, nj))
    where = jnp.stack([zj, other, x, 1 - zp]).astype(jnp.int32)
    pairs = 7 * rows * nx * rows * width
    units = (2 * nj - 1, rows, nx * rows)
    stat = (6 * nx, rows)
    gathered = (2, nx * rows, width)
    hbm = pl.BlockSpec(memory_space=pltpu.HBM)
    *offers, sent, all_q, all_g = pl.pallas_call(
        functools.partial(forward_kernel, rate, nx),
        out_shape=(jax.ShapeDtypeStruct((width, 2 * rows), BF16),) * nx
        + (jax.ShapeDtypeStruct((2 * nx, *stat), F32),)
        + (jax.ShapeDtypeStruct(gathered, BF16),) * 2,
        in_specs=[smem, hbm, hbm] + [vmem] * (2 * nx),
        out_specs=(vmem,) * (nx + 3),
        scratch_shapes=[
            pltpu.VMEM(units, F32),
            pltpu.VMEM(stat, F32),
            pltpu.VMEM((2, 2, width, nx * rows), F32),
            pltpu.VMEM((2, 2, 8, nx * rows), F32),
            pltpu.VMEM((2, 2, 8, nx * rows), F32),
            pltpu.SemaphoreType.DMA((2,)),
        ],
        compiler_params=pltpu.CompilerParams(vmem_limit_bytes=VMEM),
        cost_estimate=pl.CostEstimate(flops=4 * pairs, bytes_accessed=2 << 20, transcendentals=0),
        name="forward",
    )(where, queries, out_grad, *blocks[1:], kv)
    groups = [[z * nx + i for z in (m, (m + 1) % nz) for i in range(nx)] for m in range(1, nz, 2)]
    got = lax.all_to_all(sent, SEQ, 0, 0, axis_index_groups=groups, tiled=True)
    offers = [offers[0]] + [shifted(offers[-r % nx], "x", nx, r) for r in range(1, nx)]
    both = pl.pallas_call(
        functools.partial(backward_kernel, rate, scaling, nx),
        out_shape=(jax.ShapeDtypeStruct((width, 2 * rows), BF16),) * nx
        + (jax.ShapeDtypeStruct((rows, 2 * width), BF16),) * nj,
        in_specs=[smem] + [vmem] * 4,
        out_specs=(vmem,) * (nx + nj),
        scratch_shapes=[
            pltpu.VMEM((2, 2, width, nx * rows), F32),
            pltpu.VMEM((2, 1, nx * rows), F32),
            pltpu.VMEM((2, 1, nx * rows), F32),
            pltpu.VMEM((2, *kv.shape), F32),
            pltpu.VMEM((2, 2 * nx, rows), F32),
        ],
        compiler_params=pltpu.CompilerParams(vmem_limit_bytes=VMEM),
        cost_estimate=pl.CostEstimate(flops=10 * pairs, bytes_accessed=2 << 20, transcendentals=0),
        name="backward",
    )(where, all_q, all_g, kv, got)
    parts, dkv = both[:nx], both[nx:]
    parts = [parts[0]] + [shifted(parts[-r % nx], "x", nx, r) for r in range(1, nx)]
    dkv = [dkv[0]] + [shifted(dkv[r], "zj", nj, r) for r in range(1, nj)]
    near, far = pl.pallas_call(
        functools.partial(mix_kernel, nx),
        out_shape=(
            jax.ShapeDtypeStruct((width, rows), F32),
            jax.ShapeDtypeStruct((width, rows), BF16),
        ),
        in_specs=[smem] + [vmem] * (nx + 1),
        out_specs=(vmem,) * 2,
        compiler_params=pltpu.CompilerParams(vmem_limit_bytes=8 << 20),
        name="mix",
    )(where, got, *offers)
    back = functools.reduce(jnp.add, [p[:, rows:].astype(F32) for p in parts]).astype(BF16)
    back = swapped(jnp.concatenate([back, far], axis=1), nz)
    return pl.pallas_call(
        functools.partial(final_kernel, nx, nj),
        out_shape=(jax.ShapeDtypeStruct((rows, width), BF16),)
        + (jax.ShapeDtypeStruct((rows, width), F32),) * 3,
        in_specs=[vmem] * (nx + nj + 2),
        out_specs=(vmem,) * 4,
        compiler_params=pltpu.CompilerParams(vmem_limit_bytes=8 << 20),
        name="final",
    )(*parts, near, back, *dkv)


def solution(mesh):
    nh = mesh.shape["head"]
    split = Mesh(mesh.devices.reshape(4, 2, -1, nh), (*SEQ, "head"))
    return jax.shard_map(
        functools.partial(per_device, 4, split.shape["x"], nh),
        mesh=split,
        in_specs=(P(SEQ, "head"), P((*SEQ, "head"), None), P((*SEQ, "head"), None), P(SEQ, "head")),
        out_specs=(P(SEQ, "head"),) * 4,
        check_vma=False,
    )
```

```python
import functools
import math

import jax
import jax.numpy as jnp
from jax import lax
from jax.experimental import pallas as pl
from jax.experimental.pallas import tpu as pltpu
from jax.sharding import Mesh
from jax.sharding import PartitionSpec as P

Z = ("zj", "zp")
SEQ = (*Z, "x")
VMEM = 24 << 20
LOW = -1e30
F32 = jnp.float32
BF16 = jnp.bfloat16
NT = (((1,), (1,)), ((), ()))
TN = (((0,), (0,)), ((), ()))
NN = (((1,), (0,)), ((), ()))


def dot(a, b, dims):
    return lax.dot_general(a, b, dims, preferred_element_type=F32)


def allowed_pairs(rows, key_block, query_block):
    key_pos = lax.broadcasted_iota(jnp.int32, (rows, rows), 0) + key_block * rows
    query_pos = lax.broadcasted_iota(jnp.int32, (rows, rows), 1) + query_block * rows
    return key_pos <= query_pos


def diagonal(rows, x, nx):
    oks = [allowed_pairs(rows, x, lax.rem(x - r + nx, nx)) for r in range(nx)]
    return jnp.concatenate(oks, axis=1)


def prepare_kernel(nh, q_ref, g_ref, k_ref, v_ref, own_ref, mixed_ref, kv_ref, sems):
    width = q_ref.shape[1]
    moves = [
        pltpu.make_async_copy(k_ref, kv_ref.at[0], sems.at[0]),
        pltpu.make_async_copy(v_ref, kv_ref.at[1], sems.at[1]),
        pltpu.make_async_copy(q_ref, own_ref.at[:, :width], sems.at[2]),
        pltpu.make_async_copy(g_ref, own_ref.at[:, width:], sems.at[3]),
    ]
    for move in moves:
        move.start()
    for part in range(2):
        moves[part].wait()
        for at in range(mixed_ref.shape[0]):
            cols = slice(at % nh * width, (at % nh + 1) * width)
            mixed_ref[at, :, part * width : (part + 1) * width] = kv_ref[part, :, cols]
    moves[2].wait()
    moves[3].wait()


def gather_blocks(q_refs, query_ref, grad_ref):
    rows, width = q_refs[0].shape[0], q_refs[0].shape[1] // 2
    count = (len(q_refs) + 1) // 2
    for at, ref in enumerate(q_refs, 1):
        side, r = divmod(at, count)
        query_ref[side, r * rows : (r + 1) * rows, :] = ref[:, :width]
        grad_ref[side, r * rows : (r + 1) * rows, :] = ref[:, width:]


def each_unit(where_ref, last, unit):
    own, full = where_ref[0], where_ref[0] + where_ref[1]

    def whole(f, lane):
        side = jnp.where(f >= own, 1, 0)
        unit(f, side, f - side * own, False, lane)

    @pl.loop(0, full // 2)
    def _(i):
        whole(2 * i, 0)
        whole(2 * i + 1, 1)

    @pl.when(full % 2 == 1)
    def _():
        whole(full - 1, 0)
        unit(last, 0, own, True, 1)

    @pl.when(full % 2 == 0)
    def _():
        unit(last, 0, own, True, 0)


def folded(value, op):
    return op(value.reshape(value.shape[0] // 8, 8, value.shape[1]), axis=0)


def forward_kernel(rate, nx, where_ref, *refs):
    n = 2 * nx
    (own_q_ref, own_g_ref), q_refs, kv_ref, refs = refs[:2], refs[2 : n + 1], refs[n + 1], refs[n + 2 :]
    out_refs, (send_ref, query_ref, grad_ref), refs = refs[:nx], refs[nx : nx + 3], refs[nx + 3 :]
    s_ref, stat_ref, o_ref, m_ref, l_ref, sems = refs
    x, even = where_ref[2], where_ref[3]
    rows, width = kv_ref.shape[1], kv_ref.shape[2] // 2
    moves = [
        pltpu.make_async_copy(own_q_ref, query_ref.at[0, :rows, :], sems.at[0]),
        pltpu.make_async_copy(own_g_ref, grad_ref.at[0, :rows, :], sems.at[1]),
    ]
    for move in moves:
        move.start()
    gather_blocks(q_refs, query_ref, grad_ref)
    m_ref[...] = jnp.full_like(m_ref, LOW)
    l_ref[...] = jnp.zeros_like(l_ref)
    o_ref[...] = jnp.zeros_like(o_ref)
    for move in moves:
        move.wait()

    def score(u, side, j, masked, lane):
        s = dot(kv_ref[j, :, :width], query_ref[side], NT)
        if masked:
            s = jnp.where(diagonal(rows, x, nx), s, LOW)
        s_ref[u] = s
        m_ref[lane, side] = jnp.maximum(m_ref[lane, side], folded(s, jnp.max))

    def weigh(u, side, j, masked, lane):
        p = jnp.exp2((s_ref[u] - m_ref[0, side, 0:1, :]) * rate)
        l_ref[lane, side] += folded(p, jnp.sum)
        o_ref[lane, side] += dot(kv_ref[j, :, width:], p.astype(BF16), TN)

    last = s_ref.shape[0] - 1
    each_unit(where_ref, last, score)
    for side in range(2):
        both = jnp.maximum(m_ref[0, side], m_ref[1, side])
        m_ref[0, side, 0:1, :] = jnp.maximum(jnp.max(both, axis=0, keepdims=True), LOW / 2)
    each_unit(where_ref, last, weigh)
    for side in range(2):
        total = jnp.sum(l_ref[0, side] + l_ref[1, side], axis=0, keepdims=True)
        o_ref[0, side] += o_ref[1, side]
        grads = jnp.transpose(grad_ref[side].astype(F32))
        inner = jnp.sum(grads * o_ref[0, side], axis=0, keepdims=True)
        for r in range(nx):
            cols = slice(r * rows, (r + 1) * rows)
            at = (side ^ even) * nx + lax.rem(x - r + nx, nx)
            stat_ref[pl.ds(at, 1), :] = m_ref[0, side, 0:1, cols] * rate
            stat_ref[pl.ds(n + at, 1), :] = total[:, cols]
            stat_ref[pl.ds(2 * n + at, 1), :] = inner[:, cols]
            out_refs[r][:, side * rows : (side + 1) * rows] = o_ref[0, side, :, cols].astype(BF16)
    for to in range(n):
        send_ref[to] = stat_ref[...]


def backward_kernel(rate, scaling, nx, where_ref, *refs):
    n = 2 * nx
    (query_ref, grad_ref, kv_ref, got_ref), refs = refs[:4], refs[4:]
    nj = kv_ref.shape[0]
    out_refs, key_refs, refs = refs[:nx], refs[nx : nx + nj], refs[nx + nj :]
    dq_ref, norm_ref, delta_ref, acc_ref, row_ref = refs
    x, even = where_ref[2], where_ref[3]
    rows, width = kv_ref.shape[1], kv_ref.shape[2] // 2
    dq_ref[...] = jnp.zeros_like(dq_ref)
    acc_ref[...] = jnp.zeros_like(acc_ref)
    maxima = [got_ref[i, :n] for i in range(n)]
    top = functools.reduce(jnp.maximum, maxima)
    shares = [jnp.exp2(m - top) for m in maxima]
    total = sum(got_ref[i, n : 2 * n] * w for i, w in enumerate(shares))
    delta = sum(got_ref[i, 2 * n :] * w for i, w in enumerate(shares))
    row_ref[0] = top + jnp.log2(total)
    row_ref[1] = delta / total
    for at in range(n):
        side, r = divmod(at, nx)
        cols = slice(r * rows, (r + 1) * rows)
        row = pl.ds((side ^ even) * nx + lax.rem(x - r + nx, nx), 1)
        norm_ref[side, :, cols] = row_ref[0, row, :]
        delta_ref[side, :, cols] = row_ref[1, row, :]

    def unit(u, side, j, masked, lane):
        k, v = kv_ref[j, :, :width], kv_ref[j, :, width:]
        s = dot(k, query_ref[side], NT)
        if masked:
            s = jnp.where(diagonal(rows, x, nx), s, LOW)
        p = jnp.exp2(s * rate - norm_ref[side])
        ds = (p * (dot(v, grad_ref[side], NT) - delta_ref[side])).astype(BF16)
        acc_ref[lane, j, :, width:] += dot(p.astype(BF16), grad_ref[side], NN)
        acc_ref[lane, j, :, :width] += dot(ds, query_ref[side], NN)
        dq_ref[lane, side] += dot(k, ds, TN)

    each_unit(where_ref, 0, unit)
    for step in range(nj):
        to = lax.rem(where_ref[0] + step, nj)
        both = acc_ref[0, to] + acc_ref[1, to]
        key_refs[step][:, :width] = (both[:, :width] * scaling).astype(BF16)
        key_refs[step][:, width:] = both[:, width:].astype(BF16)
    for at in range(n):
        side, r = divmod(at, nx)
        cols = slice(r * rows, (r + 1) * rows)
        out_refs[r][:, side * rows : (side + 1) * rows] = (
            (dq_ref[0, side, :, cols] + dq_ref[1, side, :, cols]) * scaling
        ).astype(BF16)


def mix_kernel(nx, where_ref, got_ref, *refs):
    part_refs, outs = refs[:nx], refs[nx:]
    x, even = where_ref[2], where_ref[3]
    n = 2 * nx
    width, rows = part_refs[0].shape[0], part_refs[0].shape[1] // 2
    for side in range(2):
        at = (side ^ even) * nx + x
        maxima = [got_ref[i, pl.ds(at, 1), :] for i in range(n)]
        top = functools.reduce(jnp.maximum, maxima)
        sums = [got_ref[i, pl.ds(n + at, 1), :] * jnp.exp2(m - top) for i, m in enumerate(maxima)]
        total = sum(sums)
        mixed = jnp.zeros((width, rows), F32)
        for e in range(nx):
            peer = even * nx + lax.rem(x - e + nx, nx)
            share = jnp.exp2(got_ref[peer, pl.ds(at, 1), :] - top) / total
            mixed = mixed + share * part_refs[e][:, side * rows : (side + 1) * rows]
        outs[side][...] = mixed.astype(outs[side].dtype)


def final_kernel(nx, nj, *refs):
    part_refs, (near_ref, back_ref), key_refs, outs = refs[:nx], refs[nx : nx + 2], refs[nx + 2 : -4], refs[-4:]
    rows, width = outs[0].shape
    dq = back_ref[:, :rows].astype(F32)
    for part in part_refs:
        dq = dq + part[:, :rows]
    outs[0][...] = jnp.transpose(near_ref[...] + back_ref[:, rows:]).astype(BF16)
    outs[1][...] = jnp.transpose(dq)
    total = key_refs[0][...].astype(F32)
    for j in range(1, nj):
        total = total + key_refs[j][...]
    outs[2][...] = total[:, :width]
    outs[3][...] = total[:, width:]


def shifted(value, axis, count, step):
    return lax.ppermute(value, axis, [(i, (i + step) % count) for i in range(count)])


def swapped(value, count):
    pairs = [(i, (i + 1) % count) for i in range(1, count, 2)]
    return lax.ppermute(value, Z, pairs + [(j, i) for i, j in pairs])


def worked(nj, step):
    steps = [(a, (a + step) % nj, p) for a in range(nj) for p in range(2)]
    return [(2 * a + p, 2 * b + p) for a, b, p in steps if b <= a or a == p == 0]


def per_device(nj, nx, nh, queries, keys, values, out_grad):
    rows, width = queries.shape
    nz = 2 * nj
    scaling = 1.0 / math.sqrt(width)
    rate = scaling * math.log2(math.e)
    smem = pl.BlockSpec(memory_space=pltpu.SMEM)
    vmem = pl.BlockSpec(memory_space=pltpu.VMEM)
    own, mixed = pl.pallas_call(
        functools.partial(prepare_kernel, nh),
        out_shape=(
            jax.ShapeDtypeStruct((rows, 2 * width), BF16),
            jax.ShapeDtypeStruct((nj * nh, keys.shape[0], 2 * width), BF16),
        ),
        in_specs=[pl.BlockSpec(memory_space=pltpu.HBM)] * 4,
        out_specs=(vmem,) * 2,
        scratch_shapes=[pltpu.VMEM((2, *keys.shape), BF16), pltpu.SemaphoreType.DMA((4,))],
        compiler_params=pltpu.CompilerParams(vmem_limit_bytes=60 << 20),
        name="prepare",
    )(queries, out_grad, keys, values)
    other_own = swapped(own, nz)
    blocks = [own, shifted(own, "x", nx, 1)]
    blocks += [shifted(own, "x", nx, r) for r in range(2, nx)]
    blocks += [other_own] + [shifted(other_own, "x", nx, r) for r in range(1, nx)]
    kv = lax.all_to_all(mixed, ("zj", "head"), 0, 0, tiled=True)
    kv = kv.reshape(nj, rows, 2 * width)
    zj, zp, x = (lax.axis_index(a) for a in SEQ)
    other = jnp.where(zp == 0, jnp.where(zj == 0, nj, zj), lax.rem(zj + 1, nj))
    where = jnp.stack([zj, other, x, 1 - zp]).astype(jnp.int32)
    pairs = 7 * rows * nx * rows * width
    units = (2 * nj - 1, rows, nx * rows)
    stat = (6 * nx, rows)
    gathered = (2, nx * rows, width)
    hbm = pl.BlockSpec(memory_space=pltpu.HBM)
    *offers, sent, all_q, all_g = pl.pallas_call(
        functools.partial(forward_kernel, rate, nx),
        out_shape=(jax.ShapeDtypeStruct((width, 2 * rows), BF16),) * nx
        + (jax.ShapeDtypeStruct((2 * nx, *stat), F32),)
        + (jax.ShapeDtypeStruct(gathered, BF16),) * 2,
        in_specs=[smem, hbm, hbm] + [vmem] * (2 * nx),
        out_specs=(vmem,) * (nx + 3),
        scratch_shapes=[
            pltpu.VMEM(units, F32),
            pltpu.VMEM(stat, F32),
            pltpu.VMEM((2, 2, width, nx * rows), F32),
            pltpu.VMEM((2, 2, 8, nx * rows), F32),
            pltpu.VMEM((2, 2, 8, nx * rows), F32),
            pltpu.SemaphoreType.DMA((2,)),
        ],
        compiler_params=pltpu.CompilerParams(vmem_limit_bytes=VMEM),
        cost_estimate=pl.CostEstimate(flops=4 * pairs, bytes_accessed=2 << 20, transcendentals=0),
        name="forward",
    )(where, queries, out_grad, *blocks[1:], kv)
    groups = [[z * nx + i for z in (m, (m + 1) % nz) for i in range(nx)] for m in range(1, nz, 2)]
    got = lax.all_to_all(sent, SEQ, 0, 0, axis_index_groups=groups, tiled=True)
    offers = [offers[0]] + [shifted(offers[-r % nx], "x", nx, r) for r in range(1, nx)]
    both = pl.pallas_call(
        functools.partial(backward_kernel, rate, scaling, nx),
        out_shape=(jax.ShapeDtypeStruct((width, 2 * rows), BF16),) * nx
        + (jax.ShapeDtypeStruct((rows, 2 * width), BF16),) * nj,
        in_specs=[smem] + [vmem] * 4,
        out_specs=(vmem,) * (nx + nj),
        scratch_shapes=[
            pltpu.VMEM((2, 2, width, nx * rows), F32),
            pltpu.VMEM((2, 1, nx * rows), F32),
            pltpu.VMEM((2, 1, nx * rows), F32),
            pltpu.VMEM((2, *kv.shape), F32),
            pltpu.VMEM((2, 2 * nx, rows), F32),
        ],
        compiler_params=pltpu.CompilerParams(vmem_limit_bytes=VMEM),
        cost_estimate=pl.CostEstimate(flops=10 * pairs, bytes_accessed=2 << 20, transcendentals=0),
        name="backward",
    )(where, all_q, all_g, kv, got)
    parts, dkv = both[:nx], both[nx:]
    parts = [parts[0]] + [shifted(parts[-r % nx], "x", nx, r) for r in range(1, nx)]
    dkv = [dkv[0]] + [lax.ppermute(dkv[r], Z, worked(nj, r)) for r in range(1, nj)]
    near, far = pl.pallas_call(
        functools.partial(mix_kernel, nx),
        out_shape=(
            jax.ShapeDtypeStruct((width, rows), F32),
            jax.ShapeDtypeStruct((width, rows), BF16),
        ),
        in_specs=[smem] + [vmem] * (nx + 1),
        out_specs=(vmem,) * 2,
        compiler_params=pltpu.CompilerParams(vmem_limit_bytes=8 << 20),
        name="mix",
    )(where, got, *offers)
    back = functools.reduce(jnp.add, [p[:, rows:].astype(F32) for p in parts]).astype(BF16)
    back = swapped(jnp.concatenate([back, far], axis=1), nz)
    return pl.pallas_call(
        functools.partial(final_kernel, nx, nj),
        out_shape=(jax.ShapeDtypeStruct((rows, width), BF16),)
        + (jax.ShapeDtypeStruct((rows, width), F32),) * 3,
        in_specs=[vmem] * (nx + nj + 2),
        out_specs=(vmem,) * 4,
        compiler_params=pltpu.CompilerParams(vmem_limit_bytes=8 << 20),
        name="final",
    )(*parts, near, back, *dkv)


def solution(mesh):
    nh = mesh.shape["head"]
    split = Mesh(mesh.devices.reshape(4, 2, -1, nh), (*SEQ, "head"))
    return jax.shard_map(
        functools.partial(per_device, 4, split.shape["x"], nh),
        mesh=split,
        in_specs=(P(SEQ, "head"), P((*SEQ, "head"), None), P((*SEQ, "head"), None), P(SEQ, "head")),
        out_specs=(P(SEQ, "head"),) * 4,
        check_vma=False,
    )
```

```python
import functools
import math

import jax
import jax.numpy as jnp
from jax import lax
from jax.experimental import pallas as pl
from jax.experimental.pallas import tpu as pltpu
from jax.sharding import Mesh
from jax.sharding import PartitionSpec as P

SEQ = ("z", "x")
CLASSES = ((0, 1, 3, 6), (2, 4, 5, 7))
NZ = 8
VMEM = 24 << 20
LOW = -1e30
F32 = jnp.float32
BF16 = jnp.bfloat16
NT = (((1,), (1,)), ((), ()))
TN = (((0,), (0,)), ((), ()))
NN = (((1,), (0,)), ((), ()))


def dot(a, b, dims):
    return lax.dot_general(a, b, dims, preferred_element_type=F32)


def allowed_pairs(rows, key_block, query_block):
    key_pos = lax.broadcasted_iota(jnp.int32, (rows, rows), 0) + key_block * rows
    query_pos = lax.broadcasted_iota(jnp.int32, (rows, rows), 1) + query_block * rows
    return key_pos <= query_pos


def diagonal(rows, x, nx):
    oks = [allowed_pairs(rows, x, lax.rem(x - r + nx, nx)) for r in range(nx)]
    return jnp.concatenate(oks, axis=1)


def prepare_kernel(nh, q_ref, g_ref, k_ref, v_ref, own_ref, mixed_ref, kv_ref, sems):
    width = q_ref.shape[1]
    moves = [
        pltpu.make_async_copy(k_ref, kv_ref.at[0], sems.at[0]),
        pltpu.make_async_copy(v_ref, kv_ref.at[1], sems.at[1]),
        pltpu.make_async_copy(q_ref, own_ref.at[:, :width], sems.at[2]),
        pltpu.make_async_copy(g_ref, own_ref.at[:, width:], sems.at[3]),
    ]
    for move in moves:
        move.start()
    for part in range(2):
        moves[part].wait()
        for at in range(mixed_ref.shape[0]):
            cols = slice(at % nh * width, (at % nh + 1) * width)
            mixed_ref[at, :, part * width : (part + 1) * width] = kv_ref[part, :, cols]
    moves[2].wait()
    moves[3].wait()


def gather_blocks(q_refs, query_ref, grad_ref):
    rows, width = q_refs[0].shape[0], q_refs[0].shape[1] // 2
    count = (len(q_refs) + 1) // 2
    for at, ref in enumerate(q_refs, 1):
        side, r = divmod(at, count)
        query_ref[side, r * rows : (r + 1) * rows, :] = ref[:, :width]
        grad_ref[side, r * rows : (r + 1) * rows, :] = ref[:, width:]


def each_unit(own, other, last, unit):
    full = own + other

    def whole(f, lane):
        side = jnp.where(f >= own, 1, 0)
        unit(f, side, f - side * own, False, lane)

    @pl.loop(0, full // 2)
    def _(i):
        whole(2 * i, 0)
        whole(2 * i + 1, 1)

    @pl.when(full % 2 == 1)
    def _():
        whole(full - 1, 0)
        unit(last, 0, own, True, 1)

    @pl.when(full % 2 == 0)
    def _():
        unit(last, 0, own, True, 0)


def folded(value, op):
    return op(value.reshape(value.shape[0] // 8, 8, value.shape[1]), axis=0)


def paired(z):
    return (z + 1 if z % 2 else z - 1) % NZ


def class_of(z):
    return next(members for members in CLASSES if z in members)


def below(z, other):
    return sum(k < other for k in class_of(z))


def place(where_ref):
    z, own, other = where_ref[0], jnp.int32(0), jnp.int32(0)
    for at in range(NZ):
        own = jnp.where(z == at, below(at, at), own)
        other = jnp.where(z == at, below(at, paired(at)), other)
    return own, other, where_ref[1], 1 - lax.rem(z, 2)


def forward_kernel(rate, nx, where_ref, *refs):
    n = 2 * nx
    (own_q_ref, own_g_ref), q_refs, kv_ref, refs = refs[:2], refs[2 : n + 1], refs[n + 1], refs[n + 2 :]
    out_refs, (send_ref, query_ref, grad_ref), refs = refs[:nx], refs[nx : nx + 3], refs[nx + 3 :]
    s_ref, stat_ref, o_ref, m_ref, l_ref, sems = refs
    own, other, x, even = place(where_ref)
    rows, width = kv_ref.shape[1], kv_ref.shape[2] // 2
    moves = [
        pltpu.make_async_copy(own_q_ref, query_ref.at[0, :rows, :], sems.at[0]),
        pltpu.make_async_copy(own_g_ref, grad_ref.at[0, :rows, :], sems.at[1]),
    ]
    for move in moves:
        move.start()
    gather_blocks(q_refs, query_ref, grad_ref)
    m_ref[...] = jnp.full_like(m_ref, LOW)
    l_ref[...] = jnp.zeros_like(l_ref)
    o_ref[...] = jnp.zeros_like(o_ref)
    for move in moves:
        move.wait()

    def score(u, side, j, masked, lane):
        s = dot(kv_ref[j, :, :width], query_ref[side], NT)
        if masked:
            s = jnp.where(diagonal(rows, x, nx), s, LOW)
        s_ref[u] = s
        m_ref[lane, side] = jnp.maximum(m_ref[lane, side], folded(s, jnp.max))

    def weigh(u, side, j, masked, lane):
        p = jnp.exp2((s_ref[u] - m_ref[0, side, 0:1, :]) * rate)
        l_ref[lane, side] += folded(p, jnp.sum)
        o_ref[lane, side] += dot(kv_ref[j, :, width:], p.astype(BF16), TN)

    last = s_ref.shape[0] - 1
    each_unit(own, other, last, score)
    for side in range(2):
        both = jnp.maximum(m_ref[0, side], m_ref[1, side])
        m_ref[0, side, 0:1, :] = jnp.maximum(jnp.max(both, axis=0, keepdims=True), LOW / 2)
    each_unit(own, other, last, weigh)
    for side in range(2):
        total = jnp.sum(l_ref[0, side] + l_ref[1, side], axis=0, keepdims=True)
        o_ref[0, side] += o_ref[1, side]
        grads = jnp.transpose(grad_ref[side].astype(F32))
        inner = jnp.sum(grads * o_ref[0, side], axis=0, keepdims=True)
        for r in range(nx):
            cols = slice(r * rows, (r + 1) * rows)
            at = (side ^ even) * nx + lax.rem(x - r + nx, nx)
            stat_ref[pl.ds(at, 1), :] = m_ref[0, side, 0:1, cols] * rate
            stat_ref[pl.ds(n + at, 1), :] = total[:, cols]
            stat_ref[pl.ds(2 * n + at, 1), :] = inner[:, cols]
            out_refs[r][:, side * rows : (side + 1) * rows] = o_ref[0, side, :, cols].astype(BF16)
    for to in range(n):
        send_ref[to] = stat_ref[...]


def backward_kernel(rate, scaling, nx, where_ref, *refs):
    n = 2 * nx
    (query_ref, grad_ref, kv_ref, got_ref), refs = refs[:4], refs[4:]
    nj = kv_ref.shape[0]
    out_refs, key_refs, refs = refs[:nx], refs[nx : nx + nj], refs[nx + nj :]
    dq_ref, norm_ref, delta_ref, acc_ref, row_ref = refs
    own, other, x, even = place(where_ref)
    rows, width = kv_ref.shape[1], kv_ref.shape[2] // 2
    dq_ref[...] = jnp.zeros_like(dq_ref)
    acc_ref[...] = jnp.zeros_like(acc_ref)
    maxima = [got_ref[i, :n] for i in range(n)]
    top = functools.reduce(jnp.maximum, maxima)
    shares = [jnp.exp2(m - top) for m in maxima]
    total = sum(got_ref[i, n : 2 * n] * w for i, w in enumerate(shares))
    delta = sum(got_ref[i, 2 * n :] * w for i, w in enumerate(shares))
    row_ref[0] = top + jnp.log2(total)
    row_ref[1] = delta / total
    for at in range(n):
        side, r = divmod(at, nx)
        cols = slice(r * rows, (r + 1) * rows)
        row = pl.ds((side ^ even) * nx + lax.rem(x - r + nx, nx), 1)
        norm_ref[side, :, cols] = row_ref[0, row, :]
        delta_ref[side, :, cols] = row_ref[1, row, :]

    def unit(u, side, j, masked, lane):
        k, v = kv_ref[j, :, :width], kv_ref[j, :, width:]
        s = dot(k, query_ref[side], NT)
        if masked:
            s = jnp.where(diagonal(rows, x, nx), s, LOW)
        p = jnp.exp2(s * rate - norm_ref[side])
        ds = (p * (dot(v, grad_ref[side], NT) - delta_ref[side])).astype(BF16)
        acc_ref[lane, j, :, width:] += dot(p.astype(BF16), grad_ref[side], NN)
        acc_ref[lane, j, :, :width] += dot(ds, query_ref[side], NN)
        dq_ref[lane, side] += dot(k, ds, TN)

    each_unit(own, other, 0, unit)
    for step in range(nj):
        to = lax.rem(own + step, nj)
        both = acc_ref[0, to] + acc_ref[1, to]
        key_refs[step][:, :width] = (both[:, :width] * scaling).astype(BF16)
        key_refs[step][:, width:] = both[:, width:].astype(BF16)
    for at in range(n):
        side, r = divmod(at, nx)
        cols = slice(r * rows, (r + 1) * rows)
        out_refs[r][:, side * rows : (side + 1) * rows] = (
            (dq_ref[0, side, :, cols] + dq_ref[1, side, :, cols]) * scaling
        ).astype(BF16)


def mix_kernel(nx, where_ref, got_ref, *refs):
    part_refs, outs = refs[:nx], refs[nx:]
    _, _, x, even = place(where_ref)
    n = 2 * nx
    width, rows = part_refs[0].shape[0], part_refs[0].shape[1] // 2
    for side in range(2):
        at = (side ^ even) * nx + x
        maxima = [got_ref[i, pl.ds(at, 1), :] for i in range(n)]
        top = functools.reduce(jnp.maximum, maxima)
        sums = [got_ref[i, pl.ds(n + at, 1), :] * jnp.exp2(m - top) for i, m in enumerate(maxima)]
        total = sum(sums)
        mixed = jnp.zeros((width, rows), F32)
        for e in range(nx):
            peer = even * nx + lax.rem(x - e + nx, nx)
            share = jnp.exp2(got_ref[peer, pl.ds(at, 1), :] - top) / total
            mixed = mixed + share * part_refs[e][:, side * rows : (side + 1) * rows]
        outs[side][...] = mixed.astype(outs[side].dtype)


def final_kernel(nx, nj, *refs):
    part_refs, (near_ref, back_ref), key_refs, outs = refs[:nx], refs[nx : nx + 2], refs[nx + 2 : -4], refs[-4:]
    rows, width = outs[0].shape
    dq = back_ref[:, :rows].astype(F32)
    for part in part_refs:
        dq = dq + part[:, :rows]
    outs[0][...] = jnp.transpose(near_ref[...] + back_ref[:, rows:]).astype(BF16)
    outs[1][...] = jnp.transpose(dq)
    total = key_refs[0][...].astype(F32)
    for j in range(1, nj):
        total = total + key_refs[j][...]
    outs[2][...] = total[:, :width]
    outs[3][...] = total[:, width:]


def shifted(value, axis, count, step):
    return lax.ppermute(value, axis, [(i, (i + step) % count) for i in range(count)])


def swapped(value):
    return lax.ppermute(value, "z", [(z, paired(z)) for z in range(NZ)])


def worked(step):
    pairs = []
    for z in range(NZ):
        members = class_of(z)
        to = members[(members.index(z) + step) % len(members)]
        if to <= max(z, paired(z)):
            pairs.append((z, to))
    return pairs


def per_device(nj, nx, nh, queries, keys, values, out_grad):
    rows, width = queries.shape
    scaling = 1.0 / math.sqrt(width)
    rate = scaling * math.log2(math.e)
    smem = pl.BlockSpec(memory_space=pltpu.SMEM)
    vmem = pl.BlockSpec(memory_space=pltpu.VMEM)
    own, mixed = pl.pallas_call(
        functools.partial(prepare_kernel, nh),
        out_shape=(
            jax.ShapeDtypeStruct((rows, 2 * width), BF16),
            jax.ShapeDtypeStruct((nj * nh, keys.shape[0], 2 * width), BF16),
        ),
        in_specs=[pl.BlockSpec(memory_space=pltpu.HBM)] * 4,
        out_specs=(vmem,) * 2,
        scratch_shapes=[pltpu.VMEM((2, *keys.shape), BF16), pltpu.SemaphoreType.DMA((4,))],
        compiler_params=pltpu.CompilerParams(vmem_limit_bytes=60 << 20),
        name="prepare",
    )(queries, out_grad, keys, values)
    other_own = swapped(own)
    blocks = [own, shifted(own, "x", nx, 1)]
    blocks += [shifted(own, "x", nx, r) for r in range(2, nx)]
    blocks += [other_own] + [shifted(other_own, "x", nx, r) for r in range(1, nx)]
    peers = [[z * nh + h for z in members for h in range(nh)] for members in CLASSES]
    kv = lax.all_to_all(
        mixed, ("z", "head"), 0, 0, axis_index_groups=peers, tiled=True
    )
    kv = kv.reshape(nj, rows, 2 * width)
    where = jnp.stack([lax.axis_index(a) for a in SEQ]).astype(jnp.int32)
    pairs = 7 * rows * nx * rows * width
    units = (2 * nj - 1, rows, nx * rows)
    stat = (6 * nx, rows)
    gathered = (2, nx * rows, width)
    hbm = pl.BlockSpec(memory_space=pltpu.HBM)
    *offers, sent, all_q, all_g = pl.pallas_call(
        functools.partial(forward_kernel, rate, nx),
        out_shape=(jax.ShapeDtypeStruct((width, 2 * rows), BF16),) * nx
        + (jax.ShapeDtypeStruct((2 * nx, *stat), F32),)
        + (jax.ShapeDtypeStruct(gathered, BF16),) * 2,
        in_specs=[smem, hbm, hbm] + [vmem] * (2 * nx),
        out_specs=(vmem,) * (nx + 3),
        scratch_shapes=[
            pltpu.VMEM(units, F32),
            pltpu.VMEM(stat, F32),
            pltpu.VMEM((2, 2, width, nx * rows), F32),
            pltpu.VMEM((2, 2, 8, nx * rows), F32),
            pltpu.VMEM((2, 2, 8, nx * rows), F32),
            pltpu.SemaphoreType.DMA((2,)),
        ],
        compiler_params=pltpu.CompilerParams(vmem_limit_bytes=VMEM),
        cost_estimate=pl.CostEstimate(flops=4 * pairs, bytes_accessed=2 << 20, transcendentals=0),
        name="forward",
    )(where, queries, out_grad, *blocks[1:], kv)
    groups = [
        [z * nx + i for z in (m, paired(m)) for i in range(nx)] for m in range(1, NZ, 2)
    ]
    got = lax.all_to_all(sent, SEQ, 0, 0, axis_index_groups=groups, tiled=True)
    offers = [offers[0]] + [shifted(offers[-r % nx], "x", nx, r) for r in range(1, nx)]
    both = pl.pallas_call(
        functools.partial(backward_kernel, rate, scaling, nx),
        out_shape=(jax.ShapeDtypeStruct((width, 2 * rows), BF16),) * nx
        + (jax.ShapeDtypeStruct((rows, 2 * width), BF16),) * nj,
        in_specs=[smem] + [vmem] * 4,
        out_specs=(vmem,) * (nx + nj),
        scratch_shapes=[
            pltpu.VMEM((2, 2, width, nx * rows), F32),
            pltpu.VMEM((2, 1, nx * rows), F32),
            pltpu.VMEM((2, 1, nx * rows), F32),
            pltpu.VMEM((2, *kv.shape), F32),
            pltpu.VMEM((2, 2 * nx, rows), F32),
        ],
        compiler_params=pltpu.CompilerParams(vmem_limit_bytes=VMEM),
        cost_estimate=pl.CostEstimate(flops=10 * pairs, bytes_accessed=2 << 20, transcendentals=0),
        name="backward",
    )(where, all_q, all_g, kv, got)
    parts, dkv = both[:nx], both[nx:]
    parts = [parts[0]] + [shifted(parts[-r % nx], "x", nx, r) for r in range(1, nx)]
    dkv = [dkv[0]] + [lax.ppermute(dkv[r], "z", worked(r)) for r in range(nj - 1, 0, -1)]
    near, far = pl.pallas_call(
        functools.partial(mix_kernel, nx),
        out_shape=(
            jax.ShapeDtypeStruct((width, rows), F32),
            jax.ShapeDtypeStruct((width, rows), BF16),
        ),
        in_specs=[smem] + [vmem] * (nx + 1),
        out_specs=(vmem,) * 2,
        compiler_params=pltpu.CompilerParams(vmem_limit_bytes=8 << 20),
        name="mix",
    )(where, got, *offers)
    back = functools.reduce(jnp.add, [p[:, rows:].astype(F32) for p in parts])
    back = swapped(jnp.concatenate([back.astype(BF16), far], axis=1))
    return pl.pallas_call(
        functools.partial(final_kernel, nx, nj),
        out_shape=(jax.ShapeDtypeStruct((rows, width), BF16),)
        + (jax.ShapeDtypeStruct((rows, width), F32),) * 3,
        in_specs=[vmem] * (nx + nj + 2),
        out_specs=(vmem,) * 4,
        compiler_params=pltpu.CompilerParams(vmem_limit_bytes=8 << 20),
        name="final",
    )(*parts, near, back, *dkv)


def solution(mesh):
    nh = mesh.shape["head"]
    split = Mesh(mesh.devices.reshape(NZ, -1, nh), (*SEQ, "head"))
    return jax.shard_map(
        functools.partial(per_device, len(CLASSES[0]), split.shape["x"], nh),
        mesh=split,
        in_specs=(P(SEQ, "head"), P((*SEQ, "head"), None), P((*SEQ, "head"), None), P(SEQ, "head")),
        out_specs=(P(SEQ, "head"),) * 4,
        check_vma=False,
    )
```
